32 devices in a mesh: face: 16 (over z, y, core), sub: 2 (over x).
Axes of the slice: x: 2, y: 2, z: 4, core: 2. Of those that a mesh axis runs over, the one named last changes fastest.
Arguments:
- prognostic: bfloat16 [3, 2048, 16, 128], P(None, ('face', 'sub')), may hold values from -4 to 4
- metric: float32 [4, 2048, 16], P(None, ('face', 'sub')), may hold values from -0.35 to 1.6, as said below
- coriolis: float32 [2048, 16], P(('face', 'sub')), may hold values from -1.5 to 1.5
- node_point: int32 [2048, 16], P(('face', 'sub')), may hold values from 0 to 678, as said below
- send_point: int32 [6784], P(('face', 'sub')), may hold values from 0 to 678, as said below
- recv_point: int32 [6784], P(('face', 'sub')), may hold values from 0 to 678, as said below
Outputs:
- advanced: bfloat16 [3, 2048, 16, 128], P(None, ('face', 'sub'))
The draws below stay inside these ranges and needn't reach their ends.
Inputs may be any that keep to these rules, and one draw needn't show every extreme that they name: `node_point`: each device's numbers are its 679 local points; element nodes that are the same point of the surface on one device carry the same number. `send_point`: on every device the 212 slots form groups in this order: 7 slots of offset +1, 7 of offset -1, 97 of offset +8, 97 of offset -8, then one slot each of offsets 8 + 1, -8 - 1, 7, 1 - 8. A slot names the sender's point that the device at curve index d + o, taken modulo 32, shares. Every slot is used. `recv_point`: slot s of device d names the local point that is the same surface point as the sender's slot s, the sender being the device at d minus the slot's group offset modulo 32. The copies of every shared point are linked between every two devices that hold them. `metric`: entries 0 and 3 lie in [0.6, 1.6], entries 1 and 2 in [-0.35, 0.35].
All inputs are finite; a program needn't handle non-finite values.
Results may differ from the reference program's by a relative error of at most 0.007.
Values sent between devices are 32-bit elements; how exact they have to be, the bound alone decides.
No kernel may reach another device: no remote copies, remote signals or barrier semaphores. Data moves between devices by JAX's collectives and lax.ppermute only.
A program may use at most 64 MiB of HBM per device.

```python
import math
import jax
import jax.numpy as jnp
import numpy as np
from jax import lax

BX = 32
BY = 2
LEV = 128
ELEMS = 64
BLOCKS = 32
ELEMENTS = 2048
LAP = 8
PTS = 679
LINKS = 212


def link_grid_points():
    grid_width = 3 * BX + 1
    grid_height = 3 * BY + 1
    sender = []
    receiver = []
    for height in range(grid_height):
        sender.append(height * grid_width + 3 * BX)
        receiver.append(height * grid_width)
    for height in range(grid_height):
        sender.append(height * grid_width)
        receiver.append(height * grid_width + 3 * BX)
    for column in range(grid_width):
        sender.append(3 * BY * grid_width + column)
        receiver.append(column)
    for column in range(grid_width):
        sender.append(column)
        receiver.append(3 * BY * grid_width + column)
    sender.append(3 * BY * grid_width + 3 * BX)
    receiver.append(0)
    sender.append(0)
    receiver.append(3 * BY * grid_width + 3 * BX)
    sender.append(3 * BY * grid_width)
    receiver.append(3 * BX)
    sender.append(3 * BX)
    receiver.append(3 * BY * grid_width)
    return (np.array(sender, np.int32), np.array(receiver, np.int32))


def mesh_tables(key):
    base = jax.random.fold_in(key, 4242)
    key_elem, key_rot, key_point = jax.random.split(base, 3)
    elements = BX * BY
    placement_order = jax.vmap(lambda sub_key: jax.random.permutation(sub_key, elements))(jax.random.split(key_elem, BLOCKS)).astype(jnp.int32)
    rotation = jax.random.randint(key_rot, (BLOCKS, elements), 0, 4).astype(jnp.int32)[..., None]
    relabel = jax.vmap(lambda sub_key: jax.random.permutation(sub_key, PTS))(jax.random.split(key_point, BLOCKS)).astype(jnp.int32)
    across = placement_order % BX
    upward = placement_order // BX
    node_index = jnp.arange(16, dtype=jnp.int32)
    node_row = node_index // 4
    node_col = node_index % 4
    rot_col = jnp.where(rotation == 0, node_col, jnp.where(rotation == 1, 3 - node_row, jnp.where(rotation == 2, 3 - node_col, node_row)))
    rot_row = jnp.where(rotation == 0, node_row, jnp.where(rotation == 1, node_col, jnp.where(rotation == 2, 3 - node_row, 3 - node_col)))
    grid_index = (3 * upward[..., None] + rot_row) * (3 * BX + 1) + 3 * across[..., None] + rot_col
    node_table = jnp.take_along_axis(relabel, grid_index.reshape(BLOCKS, elements * 16).astype(jnp.int32), axis=1)
    sender, receiver = link_grid_points()
    send_table = relabel[:, jnp.asarray(sender)].reshape(-1).astype(jnp.int32)
    recv_table = relabel[:, jnp.asarray(receiver)].reshape(-1).astype(jnp.int32)
    return (node_table.reshape(ELEMENTS, 16).astype(jnp.int32), send_table, recv_table)


def draw_node_point(key, part):
    return mesh_tables(key)[0]


def draw_send_point(key, part):
    return mesh_tables(key)[1]


def draw_recv_point(key, part):
    return mesh_tables(key)[2]


def draw_metric(key, part):
    key_diag, key_off = jax.random.split(jax.random.fold_in(key, 17), 2)
    diagonal = jnp.exp(jax.random.uniform(key_diag, (2, ELEMENTS, 16), jnp.float32, math.log(0.6), math.log(1.6)))
    off_diag = jax.random.uniform(key_off, (2, ELEMENTS, 16), jnp.float32, -0.35, 0.35)
    diagonal = jnp.clip(diagonal, 0.6, 1.6)
    return jnp.stack([diagonal[0], off_diag[0], off_diag[1], diagonal[1]]).astype(jnp.float32)


def block_levels(own_key, shape, cuts, least, high):
    level, own = 1.0, jax.random.fold_in(own_key, 6)
    for position, parts in cuts:
        heights = jnp.exp(jax.random.uniform(jax.random.fold_in(own, position), (parts,), jnp.float32, least / len(cuts), high / len(cuts)))
        level = level * jnp.repeat(heights, shape[position] // parts).reshape([-1 if axis == position else 1 for axis in range(len(shape))])
    return level


def gaussian(own_key, dims, spread, most, cuts=(), held_as=jnp.bfloat16):
    loudness = block_levels(own_key, dims, cuts, -0.22, 0.18) if cuts else 1.0
    values = jax.random.normal(own_key, dims, jnp.float32) * spread * loudness
    return jnp.minimum(jnp.maximum(values, -most), most).astype(held_as)


def setup_inputs(seed: int = 0) -> dict:
    streams_of = jax.random.split(jax.random.key(seed), 7)
    prognostic = gaussian(streams_of[0], (3, ELEMENTS, 16, LEV), 1.0, 4.0, ((1, 32),))
    metric = draw_metric(jax.random.fold_in(streams_of[6], 71), 0)
    coriolis = jnp.clip(jax.random.uniform(streams_of[2], (ELEMENTS, 16), jnp.float32, -1.5, 1.5) * block_levels(streams_of[2], (ELEMENTS, 16), ((0, 32),), -0.4, 0.0), -1.5, 1.5)
    node_point = draw_node_point(jax.random.fold_in(streams_of[6], 71), 0)
    send_point = draw_send_point(jax.random.fold_in(streams_of[6], 71), 0)
    recv_point = draw_recv_point(jax.random.fold_in(streams_of[6], 71), 0)
    return dict(prognostic=prognostic, metric=metric, coriolis=coriolis, node_point=node_point, send_point=send_point, recv_point=recv_point)


STEP_SIZE = 0.1

def gll_tables():
    abscissa = np.array([-1.0, -math.sqrt(0.2), math.sqrt(0.2), 1.0])
    legendre = 0.5 * (5.0 * abscissa * abscissa * abscissa - 3.0 * abscissa)
    derivative = np.zeros((4, 4))
    for target in range(4):
        for source in range(4):
            if target != source:
                derivative[target, source] = legendre[target] / (legendre[source] * (abscissa[target] - abscissa[source]))
    derivative[0, 0] = -3.0
    derivative[3, 3] = 3.0
    weights = np.array([1.0, 5.0, 5.0, 1.0]) / 6.0
    return (derivative, weights)

def along_cols(values, derivative):
    return jnp.einsum('aj,erjl->eral', derivative, values, precision=lax.Precision.HIGHEST)

def along_rows(values, derivative):
    return jnp.einsum('aj,ejcl->eacl', derivative, values, precision=lax.Precision.HIGHEST)

def element_tendency(fields, metric, coriolis):
    elements = fields.shape[1]
    levels = fields.shape[3]
    deriv_table, weight_table = gll_tables()
    derivative = jnp.asarray(deriv_table, dtype=jnp.float32)
    weights = jnp.asarray(weight_table, dtype=jnp.float32)
    shaped = fields.reshape(3, elements, 4, 4, levels)
    veloc_one = shaped[0]
    veloc_two = shaped[1]
    geopot = shaped[2]
    inverse = metric.reshape(4, elements, 4, 4, 1)
    inv_aa = inverse[0]
    inv_ab = inverse[1]
    inv_ba = inverse[2]
    inv_bb = inverse[3]
    jacobian_inv = inv_aa * inv_bb - inv_ab * inv_ba
    energy = 0.5 * (veloc_one * veloc_one + veloc_two * veloc_two) + geopot
    ref_one = along_cols(energy, derivative)
    ref_two = along_rows(energy, derivative)
    grad_one = inv_aa * ref_one + inv_ba * ref_two
    grad_two = inv_ab * ref_one + inv_bb * ref_two
    cov_one = (inv_bb * veloc_one - inv_ba * veloc_two) / jacobian_inv
    cov_two = (inv_aa * veloc_two - inv_ab * veloc_one) / jacobian_inv
    vorticity = jacobian_inv * (along_cols(cov_two, derivative) - along_rows(cov_one, derivative))
    absolute = vorticity + coriolis.reshape(elements, 4, 4, 1)
    flux_one = geopot * veloc_one
    flux_two = geopot * veloc_two
    contra_one = (inv_aa * flux_one + inv_ab * flux_two) / jacobian_inv
    contra_two = (inv_ba * flux_one + inv_bb * flux_two) / jacobian_inv
    divergence = jacobian_inv * (along_cols(contra_one, derivative) + along_rows(contra_two, derivative))
    tendency = jnp.stack([absolute * veloc_two - grad_one, -absolute * veloc_one - grad_two, -divergence])
    mass_weight = (weights[:, None] * weights[None, :])[None] / jacobian_inv[..., 0]
    return (tendency.reshape(3, elements, 16, levels), mass_weight.reshape(elements, 16))

def link_groups(lap_blocks):
    side_points = 3 * BY + 1
    top_points = 3 * BX + 1
    group_sizes = [(1, side_points), (-1, side_points), (lap_blocks, top_points), (-lap_blocks, top_points), (lap_blocks + 1, 1), (-lap_blocks - 1, 1), (lap_blocks - 1, 1), (1 - lap_blocks, 1)]
    groups = []
    first_slot = 0
    for offset, slot_count in group_sizes:
        groups.append((offset, first_slot, slot_count))
        first_slot = first_slot + slot_count
    return groups

def block_terms(prognostic, metric, coriolis, node_point, device_index):
    first_elem = (device_index * ELEMS).astype(jnp.int32)
    fields = lax.dynamic_slice_in_dim(prognostic, first_elem, ELEMS, 1).astype(jnp.float32)
    local_metric = lax.dynamic_slice_in_dim(metric, first_elem, ELEMS, 1)
    local_coriolis = lax.dynamic_slice_in_dim(coriolis, first_elem, ELEMS, 0)
    point_ids = lax.dynamic_slice_in_dim(node_point, first_elem, ELEMS, 0).reshape(-1)
    tendency, mass_weight = element_tendency(fields, local_metric, local_coriolis)
    weighted = (tendency * mass_weight[None, :, :, None]).reshape(3, ELEMS * 16, LEV)
    partial_value = jnp.zeros((3, PTS, LEV), jnp.float32).at[:, point_ids, :].add(weighted)
    weight = jnp.zeros((PTS,), jnp.float32).at[point_ids].add(mass_weight.reshape(-1))
    return (fields, point_ids, partial_value, weight)

def reference(prognostic, metric, coriolis, node_point, send_point, recv_point):
    device_list = jnp.arange(BLOCKS, dtype=jnp.int32)

    def outgoing_of(device_index):
        fields, point_ids, partial_value, weight = block_terms(prognostic, metric, coriolis, node_point, device_index)
        link_ids = lax.dynamic_slice_in_dim(send_point, (device_index * LINKS).astype(jnp.int32), LINKS, 0)
        return (partial_value[:, link_ids, :], weight[link_ids])
    sent_values, sent_weight = lax.map(outgoing_of, device_list)
    groups = link_groups(LAP)

    def advance(device_index, collected):
        fields, point_ids, partial_value, weight = block_terms(prognostic, metric, coriolis, node_point, device_index)
        link_ids = lax.dynamic_slice_in_dim(recv_point, (device_index * LINKS).astype(jnp.int32), LINKS, 0)
        arrived_values = []
        arrived_weight = []
        for offset, first_slot, slot_count in groups:
            source = jnp.mod(device_index - offset, BLOCKS).astype(jnp.int32)
            values_from = lax.dynamic_index_in_dim(sent_values, source, 0, keepdims=False)
            weight_from = lax.dynamic_index_in_dim(sent_weight, source, 0, keepdims=False)
            arrived_values.append(values_from[:, first_slot:first_slot + slot_count, :])
            arrived_weight.append(weight_from[first_slot:first_slot + slot_count])
        total = partial_value.at[:, link_ids, :].add(jnp.concatenate(arrived_values, axis=1))
        total_weight = weight.at[link_ids].add(jnp.concatenate(arrived_weight, axis=0))
        averaged = total[:, point_ids, :] / total_weight[point_ids][None, :, None]
        advanced = (fields + STEP_SIZE * averaged.reshape(3, ELEMS, 16, LEV)).astype(jnp.bfloat16)
        first_elem = (device_index * ELEMS).astype(jnp.int32)
        return lax.dynamic_update_slice_in_dim(collected, advanced, first_elem, 1)
    result = jnp.zeros((3, ELEMENTS, 16, LEV), jnp.bfloat16)
    return lax.fori_loop(0, BLOCKS, advance, result)
```

```python
import math

import jax
import jax.numpy as jnp
import numpy as np
from jax import lax
from jax.experimental import pallas as pl
from jax.experimental.pallas import tpu as pltpu
from jax.sharding import PartitionSpec as P

STEP_SIZE = 0.1
AXES = ("face", "sub")
NODES = 16
SUB = 8
LANES = 128
MASS = 3 * LANES
MIB = 1024 * 1024


def shift(value, steps):
    count = lax.axis_size(AXES)
    return lax.ppermute(value, AXES, [(d, (d + steps) % count) for d in range(count)])


def gll_tables():
    abscissa = np.array([-1.0, -math.sqrt(0.2), math.sqrt(0.2), 1.0])
    legendre = 0.5 * (5.0 * abscissa * abscissa * abscissa - 3.0 * abscissa)
    derivative = np.zeros((4, 4))
    for target in range(4):
        for source in range(4):
            if target != source:
                derivative[target, source] = legendre[target] / (
                    legendre[source] * (abscissa[target] - abscissa[source])
                )
    derivative[0, 0] = -3.0
    derivative[3, 3] = 3.0
    weights = np.array([1.0, 5.0, 5.0, 1.0]) / 6.0
    return (derivative, weights)


class Plan:
    def __init__(self, elements, links, lap):
        around = (links - 8) // 6
        short = 1
        while short * (around - short) < elements:
            short += 1
        self.side = 3 * short + 1
        self.top = 3 * (around - short) + 1
        self.lap = lap
        first = [0]
        for count in (self.side, self.side, self.top, self.top, 1, 1, 1):
            first.append(first[-1] + count)
        self.first = first
        self.long_rows = -(-(self.top + 1) // SUB) * SUB
        self.side_rows = -(-(self.side + 3) // SUB) * SUB
        self.relay_rows = SUB
        self.up = 0
        self.down = self.long_rows
        self.right = 2 * self.long_rows
        self.left = self.right + self.side_rows
        self.sent_rows = self.left + self.side_rows
        self.relay_up = self.sent_rows
        self.relay_down = self.relay_up + self.relay_rows
        self.all_rows = -(-(self.relay_down + self.relay_rows) // 256) * 256

    def sent(self):
        f = self.first
        s = self.side
        return (
            (f[2], self.up, self.top),
            (f[3], self.down, self.top),
            (f[0], self.right, s),
            (f[4], self.right + s, 1),
            (f[7], self.right + s + 1, 1),
            (f[1], self.left, s),
            (f[6], self.left + s, 1),
            (f[5], self.left + s + 1, 1),
        )

    def landed(self):
        f = self.first
        s = self.side
        return (
            (f[2], self.up, self.top),
            (f[3], self.down, self.top),
            (f[0], self.right, s),
            (f[1], self.left, s),
            (f[4], self.relay_up, 1),
            (f[6], self.relay_up + 1, 1),
            (f[7], self.relay_down, 1),
            (f[5], self.relay_down + 1, 1),
        )


def iota(shape, axis):
    return lax.broadcasted_iota(jnp.int32, shape, axis)


def arranged(points_ref, moves, width):
    links = points_ref.shape[1]
    raw = points_ref[...].astype(jnp.float32)
    raw = jnp.concatenate([raw, jnp.full((1, width - links), -1.0, jnp.float32)], axis=1)
    raw = jnp.broadcast_to(raw, (SUB, width))
    lane = iota((SUB, width), 1)
    row = jnp.full((SUB, width), -1.0, jnp.float32)
    for source, target, count in moves:
        turned = pltpu.roll(raw, (target - source) % width, 1)
        row = jnp.where((lane >= target) & (lane < target + count), turned, row)
    return row[0:1]


def as_column(row, rows):
    width = row.shape[1]
    shape = (rows, width)
    return jnp.sum(jnp.where(iota(shape, 0) == iota(shape, 1), row, 0.0), axis=1, keepdims=True)


def as_row(column, width):
    shape = (column.shape[0], width)
    return jnp.sum(jnp.where(iota(shape, 0) == iota(shape, 1), column[:, :1], 0.0), axis=0, keepdims=True)


def point_rows(points):
    elements = points.shape[0]
    spread = (iota((NODES, LANES), 1) // SUB == iota((NODES, LANES), 0)).astype(jnp.float32)
    wide = jnp.dot(points, spread, precision=lax.Precision.HIGHEST, preferred_element_type=jnp.float32)
    mine = iota(wide.shape, 1) % SUB == iota(wide.shape, 0) % SUB
    return jnp.sum(jnp.where(mine, wide, 0.0).reshape(elements // SUB, SUB, LANES), axis=1)


def both_halves(mass):
    return mass + pltpu.roll(mass, LANES // 2, 1)


def split_lanes(mass):
    upper = mass.astype(jnp.bfloat16).astype(jnp.float32)
    return jnp.where(iota(mass.shape, 1) < LANES // 2, mass, mass - upper)


def derive(values, axis, scale):
    table, _ = gll_tables()
    out = [None] * NODES
    for other in range(4):
        spot = (lambda i: 4 * other + i) if axis == 1 else (lambda i: 4 * i + other)
        x0, x1, x2, x3 = (values[spot(i)] for i in range(4))
        diff_a = x0 - x3
        diff_b = x1 - x2
        even = (x0 + x3) - (x1 + x2)
        for i in (0, 1):
            factor = scale[other] * scale[i]
            p = even * np.float32(factor * 0.5 * (table[i, 0] + table[i, 3]))
            q = diff_a * np.float32(factor * 0.5 * (table[i, 0] - table[i, 3])) + diff_b * np.float32(
                factor * 0.5 * (table[i, 1] - table[i, 2])
            )
            out[spot(i)] = q + p
            out[spot(3 - i)] = q - p
    return out


def tendency_kernel(plan, prog, metric, cor, points, send, fields, weighted, up, down, right, left, *scratch):
    met_v, cor_v, pts_v, send_v, tile, mask, sems, chunk_sems = scratch
    elements = fields.shape[1]
    groups = elements // SUB
    chunks = chunk_sems.shape[0]
    per = elements // chunks
    smalls = [
        pltpu.make_async_copy(source, target, sems.at[i])
        for i, (source, target) in enumerate(((points, pts_v), (send, send_v), (metric, met_v), (cor, cor_v)))
    ]
    for copy in smalls:
        copy.start()
    larges = [
        pltpu.make_async_copy(
            prog.at[:, pl.ds(i * per, per)], fields.at[:, pl.ds(i * per, per)], chunk_sems.at[i]
        )
        for i in range(chunks)
    ]
    for copy in larges:
        copy.start()
    smalls[0].wait()
    smalls[1].wait()
    rows = plan.sent_rows
    wanted = as_column(arranged(send_v, plan.sent(), plan.all_rows), rows)
    numbers = point_rows(pts_v[...].astype(jnp.float32))
    for group in range(groups):
        mask[:, group * LANES : (group + 1) * LANES] = (
            jnp.broadcast_to(wanted, (rows, LANES)) == numbers[group : group + 1]
        ).astype(jnp.bfloat16)
    smalls[2].wait()
    smalls[3].wait()
    _, scale = gll_tables()
    node = iota((SUB, NODES), 1)
    row_edge = (node // 4 == 0) | (node // 4 == 3)
    col_edge = (node % 4 == 0) | (node % 4 == 3)
    quad = jnp.where(row_edge, np.float32(scale[0]), np.float32(scale[1])) * jnp.where(
        col_edge, np.float32(scale[0]), np.float32(scale[1])
    )

    def body(group, carry):
        here = pl.ds(group * SUB, SUB)
        a, b, e, g = (met_v[i, here, :] for i in range(4))
        inv = 1.0 / (a * g - b * e)
        mass = quad * inv
        force = mass * cor_v[here, :]

        def spread(compact):
            return [jnp.broadcast_to(compact[:, k : k + 1], (SUB, LANES)) for k in range(NODES)]

        ca, cb, ce, cg, cf, cm = (spread(v) for v in (a * inv, b * inv, e * inv, g * inv, force, mass))
        for f in range(3):
            tile[f] = fields[f, here].astype(jnp.float32).reshape(SUB * NODES, LANES)
        u, v, h = ([tile[f, pl.ds(k, SUB, stride=NODES), :] for k in range(NODES)] for f in range(3))
        span = range(NODES)
        energy = [0.5 * (u[k] * u[k] + v[k] * v[k]) + h[k] for k in span]
        along = derive(energy, 1, scale)
        across = derive(energy, 0, scale)
        grad_one = [ca[k] * along[k] + ce[k] * across[k] for k in span]
        grad_two = [cb[k] * along[k] + cg[k] * across[k] for k in span]
        turn_two = derive([ca[k] * v[k] - cb[k] * u[k] for k in span], 1, scale)
        turn_one = derive([cg[k] * u[k] - ce[k] * v[k] for k in span], 0, scale)
        eta = [turn_two[k] - turn_one[k] + cf[k] for k in span]
        flow_one = derive([h[k] * (ca[k] * u[k] + cb[k] * v[k]) for k in span], 1, scale)
        flow_two = derive([h[k] * (ce[k] * u[k] + cg[k] * v[k]) for k in span], 0, scale)
        parts = (
            [eta[k] * v[k] - grad_one[k] for k in span],
            [-(eta[k] * u[k]) - grad_two[k] for k in span],
            [-(flow_one[k] + flow_two[k]) for k in span],
            [split_lanes(cm[k]) for k in span],
        )
        there = pl.ds(group * LANES, LANES)
        for f, part in enumerate(parts):
            weighted[there, f * LANES : (f + 1) * LANES] = jnp.concatenate(part, axis=0).astype(jnp.bfloat16)
        return carry

    step = groups // chunks
    for i in range(chunks):
        larges[i].wait()
        lax.fori_loop(i * step, (i + 1) * step, body, 0)
    sums = jnp.dot(mask[...], weighted[...], preferred_element_type=jnp.float32)
    masses = both_halves(sums[:, MASS:])
    for ref, start, count, used, lane in (
        (up, plan.up, plan.long_rows, plan.top, 0),
        (down, plan.down, plan.long_rows, plan.top, 0),
        (right, plan.right, plan.side_rows, plan.side + 2, 0),
        (left, plan.left, plan.side_rows, plan.side + 2, plan.side_rows),
    ):
        ref[...] = sums[start : start + count, :MASS]
        row = as_row(masses[start : start + count], LANES)
        ref[used : used + 1, 0:LANES] = pltpu.roll(jnp.broadcast_to(row, (SUB, LANES)), lane, 1)[0:1]


def local_kernel(plan, weighted, points, recv, own, table):
    elements = points.shape[0]
    groups = elements // SUB
    values = points[...].astype(jnp.float32)
    numbers = point_rows(values)
    landing = arranged(recv, plan.landed(), plan.all_rows)
    tall = SUB * NODES

    def body(group, carry):
        part = points[pl.ds(group * SUB, SUB), :].astype(jnp.float32)
        wide = jnp.broadcast_to(part[:, None, :], (SUB, NODES, NODES)).reshape(tall, NODES)
        pick = iota((tall, NODES), 0) % NODES == iota((tall, NODES), 1)
        column = jnp.sum(jnp.where(pick, wide, 0.0), axis=1, keepdims=True)
        column = jnp.broadcast_to(column, (tall, LANES))
        here = pl.ds(group * tall, tall)
        same = jnp.concatenate(
            [(column == numbers[i : i + 1]).astype(jnp.bfloat16) for i in range(groups)], axis=1
        )
        own[here, :] = jnp.dot(same, weighted[...], preferred_element_type=jnp.float32)
        for i in range(0, plan.all_rows, LANES):
            table[here, i : i + LANES] = (column == landing[:, i : i + LANES]).astype(jnp.bfloat16)
        return carry

    lax.fori_loop(0, groups, body, 0)


def relay_kernel(plan, right, left, own, up, down):
    used = plan.side + 2
    rest = jnp.zeros((SUB - 2, MASS), jnp.float32)
    lane = iota((SUB, LANES), 1)
    first = jnp.broadcast_to(right[used : used + 1, :LANES], (SUB, LANES))
    second = jnp.broadcast_to(left[used : used + 1, :LANES], (SUB, LANES))
    begin = 2 * plan.side_rows
    for i, ref in enumerate((up, down)):
        row = plan.side + i
        ref[...] = jnp.concatenate([right[row : row + 1], left[row : row + 1], rest], axis=0)
        to = begin + i * plan.relay_rows
        masses = jnp.where(lane == to, pltpu.roll(first, to - row, 1), 0.0) + jnp.where(
            lane == to + 1, pltpu.roll(second, to + 1 - row - plan.side_rows, 1), 0.0
        )
        ref[2:3, 0:LANES] = masses[0:1]


def finish_kernel(plan, fields, own, table, up, down, right, left, relay_up, relay_down, out, held, sems):
    top = plan.top
    used = plan.side + 2
    small = right[used : used + 1, :LANES] + left[used : used + 1, :LANES]
    small = small + relay_up[2:3, :LANES] + relay_down[2:3, :LANES]
    count = 2 * plan.side_rows + 2 * plan.relay_rows
    masses = jnp.concatenate(
        [
            jnp.broadcast_to(as_column(row, rows), (rows, LANES))
            for row, rows in (
                (up[top : top + 1, :LANES], plan.long_rows),
                (down[top : top + 1, :LANES], plan.long_rows),
                (small, count),
            )
        ],
        axis=0,
    )
    landed = jnp.concatenate([ref[...] for ref in (up, down, right, left, relay_up, relay_down)], axis=0)
    landed = jnp.concatenate([landed, split_lanes(masses)], axis=1)
    spare = plan.all_rows - landed.shape[0]
    if spare:
        landed = jnp.concatenate([landed, jnp.zeros((spare, landed.shape[1]), jnp.float32)], axis=0)
    landed = landed.astype(jnp.bfloat16)
    chunks = sems.shape[0]
    elements = fields.shape[1]
    per = elements // chunks
    copies = []
    for i in range(chunks):
        rows = slice(i * per * NODES, (i + 1) * per * NODES)
        here = slice(i * per, (i + 1) * per)
        total = own[rows, :] + jnp.dot(table[rows, :], landed, preferred_element_type=jnp.float32)
        factor = np.float32(STEP_SIZE) / both_halves(total[:, MASS:])
        for f in range(3):
            moved = (total[:, f * LANES : (f + 1) * LANES] * factor).reshape(per, NODES, LANES)
            held[f, here] = (fields[f, here].astype(jnp.float32) + moved).astype(jnp.bfloat16)
        copy = pltpu.make_async_copy(
            held.at[:, pl.ds(i * per, per)], out.at[:, pl.ds(i * per, per)], sems.at[i]
        )
        copy.start()
        copies.append(copy)
    for copy in copies:
        copy.wait()


def call(kernel, name, outs, ins, args, scratch=(), limit=8 * MIB, flops=0):
    return pl.pallas_call(
        kernel,
        out_shape=[jax.ShapeDtypeStruct(shape, dtype) for shape, dtype, _ in outs],
        out_specs=[pl.BlockSpec(memory_space=space) for _, _, space in outs],
        in_specs=[pl.BlockSpec(memory_space=space) for space in ins],
        scratch_shapes=list(scratch),
        compiler_params=pltpu.CompilerParams(vmem_limit_bytes=limit),
        cost_estimate=pl.CostEstimate(flops=flops, bytes_accessed=0, transcendentals=0) if flops else None,
        name=name,
    )(*args)


def local(prognostic, metric, coriolis, node_point, send_point, recv_point):
    elements = prognostic.shape[1]
    levels = prognostic.shape[3]
    links = send_point.shape[0]
    plan = Plan(elements, links, 4 * lax.axis_size("sub"))
    rows = elements * NODES
    vm, hbm = pltpu.VMEM, pl.ANY
    f32, bf16 = jnp.float32, jnp.bfloat16
    send = send_point.reshape(1, links)
    recv = recv_point.reshape(1, links)
    long_shape = ((plan.long_rows, MASS), f32, vm)
    side_shape = ((plan.side_rows, MASS), f32, vm)
    relay_shape = ((plan.relay_rows, MASS), f32, vm)
    fields, weighted, up, down, right, left = call(
        lambda *refs: tendency_kernel(plan, *refs),
        "tendency",
        ((prognostic.shape, bf16, vm), ((rows, 4 * levels), bf16, vm), long_shape, long_shape, side_shape, side_shape),
        (hbm,) * 5,
        (prognostic, metric, coriolis, node_point, send),
        (
            vm(metric.shape, f32),
            vm(coriolis.shape, f32),
            vm(node_point.shape, jnp.int32),
            vm(send.shape, jnp.int32),
            vm((3, SUB * NODES, levels), f32),
            vm((plan.sent_rows, rows), bf16),
            pltpu.SemaphoreType.DMA((4,)),
            pltpu.SemaphoreType.DMA((4,)),
        ),
    )
    from_below = shift(up, plan.lap)
    from_above = shift(down, -plan.lap)
    from_left = shift(right, 1)
    from_right = shift(left, -1)
    own, table = call(
        lambda *refs: local_kernel(plan, *refs),
        "local",
        (((rows, 4 * levels), f32, vm), ((rows, plan.all_rows), bf16, vm)),
        (vm, vm, vm),
        (weighted, node_point, recv),
    )
    relay_up, relay_down = call(
        lambda *refs: relay_kernel(plan, *refs),
        "relay",
        (relay_shape, relay_shape),
        (vm, vm, hbm),
        (from_left, from_right, own),
    )
    corner_below = shift(relay_up, plan.lap)
    corner_above = shift(relay_down, -plan.lap)
    (advanced,) = call(
        lambda *refs: finish_kernel(plan, *refs),
        "finish",
        ((prognostic.shape, bf16, hbm),),
        (vm,) * 9,
        (fields, own, table, from_below, from_above, from_left, from_right, corner_below, corner_above),
        (vm(prognostic.shape, bf16), pltpu.SemaphoreType.DMA((4,))),
    )
    return advanced


def solution(mesh):
    placed = (
        P(None, AXES, None, None),
        P(None, AXES, None),
        P(AXES, None),
        P(AXES, None),
        P(AXES),
        P(AXES),
    )
    return jax.shard_map(
        local,
        mesh=mesh,
        in_specs=placed,
        out_specs=P(None, AXES, None, None),
        check_vma=False,
    )
```

```python
import math

import jax
import jax.numpy as jnp
import numpy as np
from jax import lax
from jax.experimental import pallas as pl
from jax.experimental.pallas import tpu as pltpu
from jax.sharding import PartitionSpec as P

STEP_SIZE = 0.1
AXES = ("face", "sub")
NODES = 16
SUB = 8
LANES = 128
MASS = 3 * LANES
MIB = 1024 * 1024


def shift(value, steps):
    count = lax.axis_size(AXES)
    return lax.ppermute(value, AXES, [(d, (d + steps) % count) for d in range(count)])


def gll_tables():
    abscissa = np.array([-1.0, -math.sqrt(0.2), math.sqrt(0.2), 1.0])
    legendre = 0.5 * (5.0 * abscissa * abscissa * abscissa - 3.0 * abscissa)
    derivative = np.zeros((4, 4))
    for target in range(4):
        for source in range(4):
            if target != source:
                derivative[target, source] = legendre[target] / (
                    legendre[source] * (abscissa[target] - abscissa[source])
                )
    derivative[0, 0] = -3.0
    derivative[3, 3] = 3.0
    weights = np.array([1.0, 5.0, 5.0, 1.0]) / 6.0
    return (derivative, weights)


class Plan:
    def __init__(self, elements, links, lap):
        around = (links - 8) // 6
        short = 1
        while short * (around - short) < elements:
            short += 1
        self.side = 3 * short + 1
        self.top = 3 * (around - short) + 1
        self.lap = lap
        first = [0]
        for count in (self.side, self.side, self.top, self.top, 1, 1, 1):
            first.append(first[-1] + count)
        self.first = first
        self.long_rows = -(-(self.top + 1) // SUB) * SUB
        self.side_rows = -(-(self.side + 3) // SUB) * SUB
        self.relay_rows = SUB
        self.up = 0
        self.down = self.long_rows
        self.right = 2 * self.long_rows
        self.left = self.right + self.side_rows
        self.sent_rows = self.left + self.side_rows
        self.relay_up = self.sent_rows
        self.relay_down = self.relay_up + self.relay_rows
        self.all_rows = -(-(self.relay_down + self.relay_rows) // 256) * 256

    def sent(self):
        f = self.first
        s = self.side
        return (
            (f[2], self.up, self.top),
            (f[3], self.down, self.top),
            (f[0], self.right, s),
            (f[4], self.right + s, 1),
            (f[7], self.right + s + 1, 1),
            (f[1], self.left, s),
            (f[6], self.left + s, 1),
            (f[5], self.left + s + 1, 1),
        )

    def landed(self):
        f = self.first
        s = self.side
        return (
            (f[2], self.up, self.top),
            (f[3], self.down, self.top),
            (f[0], self.right, s),
            (f[1], self.left, s),
            (f[4], self.relay_up, 1),
            (f[6], self.relay_up + 1, 1),
            (f[7], self.relay_down, 1),
            (f[5], self.relay_down + 1, 1),
        )


def iota(shape, axis):
    return lax.broadcasted_iota(jnp.int32, shape, axis)


def arranged(points_ref, moves, width):
    links = points_ref.shape[1]
    raw = points_ref[...].astype(jnp.float32)
    raw = jnp.concatenate([raw, jnp.full((1, width - links), -1.0, jnp.float32)], axis=1)
    raw = jnp.broadcast_to(raw, (SUB, width))
    lane = iota((SUB, width), 1)
    row = jnp.full((SUB, width), -1.0, jnp.float32)
    for source, target, count in moves:
        turned = pltpu.roll(raw, (target - source) % width, 1)
        row = jnp.where((lane >= target) & (lane < target + count), turned, row)
    return row[0:1]


def as_column(row, rows):
    width = row.shape[1]
    shape = (rows, width)
    return jnp.sum(jnp.where(iota(shape, 0) == iota(shape, 1), row, 0.0), axis=1, keepdims=True)


def as_row(column, width):
    shape = (column.shape[0], width)
    return jnp.sum(jnp.where(iota(shape, 0) == iota(shape, 1), column[:, :1], 0.0), axis=0, keepdims=True)


def point_rows(stack, first):
    elements = stack.shape[0]
    square = (LANES, LANES)
    spread = (iota(square, 1) // SUB + first == iota(square, 0)).astype(jnp.float32)
    wide = jnp.dot(stack, spread, precision=lax.Precision.HIGHEST, preferred_element_type=jnp.float32)
    mine = iota(wide.shape, 1) % SUB == iota(wide.shape, 0) % SUB
    return jnp.sum(jnp.where(mine, wide, 0.0).reshape(elements // SUB, SUB, LANES), axis=1)


def both_halves(mass):
    return mass + pltpu.roll(mass, LANES // 2, 1)


def split_lanes(mass):
    upper = mass.astype(jnp.bfloat16).astype(jnp.float32)
    return jnp.where(iota(mass.shape, 1) < LANES // 2, mass, mass - upper)


def derive(values, axis, scale):
    table, _ = gll_tables()
    out = [None] * NODES
    for other in range(4):
        spot = (lambda i: 4 * other + i) if axis == 1 else (lambda i: 4 * i + other)
        x0, x1, x2, x3 = (values[spot(i)] for i in range(4))
        diff_a = x0 - x3
        diff_b = x1 - x2
        even = (x0 + x3) - (x1 + x2)
        for i in (0, 1):
            factor = scale[other] * scale[i]
            p = even * np.float32(factor * 0.5 * (table[i, 0] + table[i, 3]))
            q = diff_a * np.float32(factor * 0.5 * (table[i, 0] - table[i, 3])) + diff_b * np.float32(
                factor * 0.5 * (table[i, 1] - table[i, 2])
            )
            out[spot(i)] = q + p
            out[spot(3 - i)] = q - p
    return out


def tendency_kernel(plan, *refs):
    prog, metric, cor, points, send, recv = refs[:6]
    fields, weighted, numbers, pts_v, recv_v, up, down, right, left = refs[6:15]
    met_v, cor_v, send_v, tile, mask, coefs, sems, chunk_sems = refs[15:]
    elements = fields.shape[1]
    groups = elements // SUB
    chunks = chunk_sems.shape[0]
    per = elements // chunks
    smalls = [
        pltpu.make_async_copy(source, target, sems.at[i])
        for i, (source, target) in enumerate(((points, pts_v), (send, send_v), (metric, met_v), (cor, cor_v)))
    ]
    for copy in smalls:
        copy.start()
    larges = [
        pltpu.make_async_copy(
            prog.at[:, pl.ds(i * per, per)], fields.at[:, pl.ds(i * per, per)], chunk_sems.at[i]
        )
        for i in range(chunks)
    ]
    for copy in larges:
        copy.start()
    later = pltpu.make_async_copy(recv, recv_v, sems.at[4])
    later.start()
    for copy in smalls:
        copy.wait()
    rows = plan.sent_rows
    wanted = as_column(arranged(send_v, plan.sent(), plan.all_rows), rows)
    _, scale = gll_tables()
    a, b, e, g = (met_v[i] for i in range(4))
    node = iota(a.shape, 0)
    row_edge = (node // 4 == 0) | (node // 4 == 3)
    col_edge = (node % 4 == 0) | (node % 4 == 3)
    quad = jnp.where(row_edge, np.float32(scale[0]), np.float32(scale[1])) * jnp.where(
        col_edge, np.float32(scale[0]), np.float32(scale[1])
    )
    inv = 1.0 / (a * g - b * e)
    mass = quad * inv
    stack = (a * inv, b * inv, e * inv, g * inv, mass * cor_v[...], mass, pts_v[...].astype(jnp.float32))
    spare = LANES - len(stack) * NODES
    stack = jnp.concatenate(stack + (jnp.zeros((spare, elements), jnp.float32),), axis=0)
    coefs[...] = jnp.transpose(stack)
    numbers[...] = point_rows(coefs[...], 6 * NODES)
    for group in range(groups):
        mask[:, group * LANES : (group + 1) * LANES] = (
            jnp.broadcast_to(wanted, (rows, LANES)) == numbers[group : group + 1, :]
        ).astype(jnp.bfloat16)

    def body(group, carry):
        here = pl.ds(group * SUB, SUB)
        compact = coefs[here, :]

        def spread(which):
            lanes = range(which * NODES, (which + 1) * NODES)
            return [jnp.broadcast_to(compact[:, k : k + 1], (SUB, LANES)) for k in lanes]

        ca, cb, ce, cg, cf, cm = (spread(i) for i in range(6))
        for f in range(3):
            tile[f] = fields[f, here].astype(jnp.float32).reshape(SUB * NODES, LANES)
        u, v, h = ([tile[f, pl.ds(k, SUB, stride=NODES), :] for k in range(NODES)] for f in range(3))
        span = range(NODES)
        energy = [0.5 * (u[k] * u[k] + v[k] * v[k]) + h[k] for k in span]
        along = derive(energy, 1, scale)
        across = derive(energy, 0, scale)
        grad_one = [ca[k] * along[k] + ce[k] * across[k] for k in span]
        grad_two = [cb[k] * along[k] + cg[k] * across[k] for k in span]
        turn_two = derive([ca[k] * v[k] - cb[k] * u[k] for k in span], 1, scale)
        turn_one = derive([cg[k] * u[k] - ce[k] * v[k] for k in span], 0, scale)
        eta = [turn_two[k] - turn_one[k] + cf[k] for k in span]
        flow_one = derive([h[k] * (ca[k] * u[k] + cb[k] * v[k]) for k in span], 1, scale)
        flow_two = derive([h[k] * (ce[k] * u[k] + cg[k] * v[k]) for k in span], 0, scale)
        parts = (
            [eta[k] * v[k] - grad_one[k] for k in span],
            [-(eta[k] * u[k]) - grad_two[k] for k in span],
            [-(flow_one[k] + flow_two[k]) for k in span],
            [split_lanes(cm[k]) for k in span],
        )
        there = pl.ds(group * LANES, LANES)
        for f, part in enumerate(parts):
            weighted[there, f * LANES : (f + 1) * LANES] = jnp.concatenate(part, axis=0).astype(jnp.bfloat16)
        return carry

    step = groups // chunks
    for i in range(chunks):
        larges[i].wait()
        lax.fori_loop(i * step, (i + 1) * step, body, 0)
    later.wait()
    sums = jnp.dot(mask[...], weighted[...], preferred_element_type=jnp.float32)
    masses = both_halves(sums[:, MASS:])
    for ref, start, count, used, lane in (
        (up, plan.up, plan.long_rows, plan.top, 0),
        (down, plan.down, plan.long_rows, plan.top, 0),
        (right, plan.right, plan.side_rows, plan.side + 2, 0),
        (left, plan.left, plan.side_rows, plan.side + 2, plan.side_rows),
    ):
        ref[...] = sums[start : start + count, :MASS]
        row = as_row(masses[start : start + count], LANES)
        ref[used : used + 1, 0:LANES] = pltpu.roll(jnp.broadcast_to(row, (SUB, LANES)), lane, 1)[0:1]


def point_columns(points, group):
    return jnp.concatenate(
        [
            jnp.broadcast_to(points[:, e : e + 1], (NODES, LANES))
            for e in range(group * SUB, (group + 1) * SUB)
        ],
        axis=0,
    )


def local_sums(points, numbers, weighted, own, first):
    groups = weighted.shape[0] // LANES
    tall = SUB * NODES
    for i in range(own.shape[0] // tall):
        column = point_columns(points, first + i)
        same = jnp.concatenate(
            [(column == numbers[j : j + 1, :]).astype(jnp.bfloat16) for j in range(groups)], axis=1
        )
        own[i * tall : (i + 1) * tall, :] = jnp.dot(same, weighted[...], preferred_element_type=jnp.float32)


def before_kernel(plan, weighted, numbers, points, recv, own, table):
    landing = arranged(recv, plan.landed(), plan.all_rows)
    values = points[...].astype(jnp.float32)
    tall = SUB * NODES
    for group in range(numbers.shape[0]):
        column = point_columns(values, group)
        for i in range(0, plan.all_rows, LANES):
            table[group * tall : (group + 1) * tall, i : i + LANES] = (
                column == landing[:, i : i + LANES]
            ).astype(jnp.bfloat16)
    local_sums(values, numbers, weighted, own, 0)


def after_kernel(first, weighted, numbers, points, order, own):
    local_sums(points[...].astype(jnp.float32), numbers, weighted, own, first)


def relay_kernel(plan, right, left, own, up, down):
    used = plan.side + 2
    rest = jnp.zeros((SUB - 2, MASS), jnp.float32)
    lane = iota((SUB, LANES), 1)
    first = jnp.broadcast_to(right[used : used + 1, :LANES], (SUB, LANES))
    second = jnp.broadcast_to(left[used : used + 1, :LANES], (SUB, LANES))
    begin = 2 * plan.side_rows
    for i, ref in enumerate((up, down)):
        row = plan.side + i
        ref[...] = jnp.concatenate([right[row : row + 1], left[row : row + 1], rest], axis=0)
        to = begin + i * plan.relay_rows
        masses = jnp.where(lane == to, pltpu.roll(first, to - row, 1), 0.0) + jnp.where(
            lane == to + 1, pltpu.roll(second, to + 1 - row - plan.side_rows, 1), 0.0
        )
        ref[2:3, 0:LANES] = masses[0:1]


def finish_kernel(plan, fields, own_a, own_b, table, up, down, right, left, relay_up, relay_down, out, held, sems):
    top = plan.top
    used = plan.side + 2
    small = right[used : used + 1, :LANES] + left[used : used + 1, :LANES]
    small = small + relay_up[2:3, :LANES] + relay_down[2:3, :LANES]
    count = 2 * plan.side_rows + 2 * plan.relay_rows
    masses = jnp.concatenate(
        [
            jnp.broadcast_to(as_column(row, rows), (rows, LANES))
            for row, rows in (
                (up[top : top + 1, :LANES], plan.long_rows),
                (down[top : top + 1, :LANES], plan.long_rows),
                (small, count),
            )
        ],
        axis=0,
    )
    landed = jnp.concatenate([ref[...] for ref in (up, down, right, left, relay_up, relay_down)], axis=0)
    landed = jnp.concatenate([landed, split_lanes(masses)], axis=1)
    spare = plan.all_rows - landed.shape[0]
    if spare:
        landed = jnp.concatenate([landed, jnp.zeros((spare, landed.shape[1]), jnp.float32)], axis=0)
    landed = landed.astype(jnp.bfloat16)
    chunks = sems.shape[0]
    elements = fields.shape[1]
    per = elements // chunks
    copies = []
    for i in range(chunks):
        rows = slice(i * per * NODES, (i + 1) * per * NODES)
        here = slice(i * per, (i + 1) * per)
        own = own_a if rows.stop <= own_a.shape[0] else own_b
        skip = 0 if own is own_a else own_a.shape[0]
        base = own[rows.start - skip : rows.stop - skip, :]
        total = base + jnp.dot(table[rows, :], landed, preferred_element_type=jnp.float32)
        factor = np.float32(STEP_SIZE) / both_halves(total[:, MASS:])
        for f in range(3):
            moved = (total[:, f * LANES : (f + 1) * LANES] * factor).reshape(per, NODES, LANES)
            held[f, here] = (fields[f, here].astype(jnp.float32) + moved).astype(jnp.bfloat16)
        copy = pltpu.make_async_copy(
            held.at[:, pl.ds(i * per, per)], out.at[:, pl.ds(i * per, per)], sems.at[i]
        )
        copy.start()
        copies.append(copy)
    for copy in copies:
        copy.wait()


def in_hbm(value):
    return pltpu.with_memory_space_constraint(value, pltpu.HBM)


def call(kernel, name, outs, ins, args, scratch=(), limit=8 * MIB, flops=0):
    return pl.pallas_call(
        kernel,
        out_shape=[jax.ShapeDtypeStruct(shape, dtype) for shape, dtype, _ in outs],
        out_specs=[pl.BlockSpec(memory_space=space) for _, _, space in outs],
        in_specs=[pl.BlockSpec(memory_space=space) for space in ins],
        scratch_shapes=list(scratch),
        compiler_params=pltpu.CompilerParams(vmem_limit_bytes=limit),
        cost_estimate=pl.CostEstimate(flops=flops, bytes_accessed=0, transcendentals=0) if flops else None,
        name=name,
    )(*args)


def local(prognostic, metric, coriolis, node_point, send_point, recv_point):
    elements = prognostic.shape[1]
    levels = prognostic.shape[3]
    links = send_point.shape[0]
    plan = Plan(elements, links, 4 * lax.axis_size("sub"))
    rows = elements * NODES
    vm, hbm = pltpu.VMEM, pltpu.HBM
    f32, bf16 = jnp.float32, jnp.bfloat16
    send = send_point.reshape(1, links)
    recv = recv_point.reshape(1, links)
    metric = jnp.transpose(metric, (0, 2, 1))
    coriolis = jnp.transpose(coriolis)
    points = jnp.transpose(node_point)
    early = rows // 4
    wide = 4 * levels
    long_shape = ((plan.long_rows, MASS), f32, vm)
    side_shape = ((plan.side_rows, MASS), f32, vm)
    relay_shape = ((plan.relay_rows, MASS), f32, vm)
    fields, weighted, numbers, points, recv, up, down, right, left = call(
        lambda *refs: tendency_kernel(plan, *refs),
        "tendency",
        (
            (prognostic.shape, bf16, vm),
            ((rows, wide), bf16, vm),
            ((elements // SUB, LANES), f32, vm),
            (points.shape, jnp.int32, vm),
            (recv.shape, jnp.int32, vm),
            long_shape,
            long_shape,
            side_shape,
            side_shape,
        ),
        (hbm,) * 6,
        tuple(in_hbm(x) for x in (prognostic, metric, coriolis, points, send, recv)),
        (
            vm(metric.shape, f32),
            vm(coriolis.shape, f32),
            vm(send.shape, jnp.int32),
            vm((3, SUB * NODES, levels), f32),
            vm((plan.sent_rows, rows), bf16),
            vm((elements, LANES), f32),
            pltpu.SemaphoreType.DMA((5,)),
            pltpu.SemaphoreType.DMA((4,)),
        ),
    )
    from_below = shift(up, plan.lap)
    from_above = shift(down, -plan.lap)
    from_left = shift(right, 1)
    from_right = shift(left, -1)
    own_a, table = call(
        lambda *refs: before_kernel(plan, *refs),
        "before",
        (((early, wide), f32, vm), ((rows, plan.all_rows), bf16, vm)),
        (vm,) * 4,
        (weighted, numbers, points, recv),
    )
    relay_up, relay_down = call(
        lambda *refs: relay_kernel(plan, *refs),
        "relay",
        (relay_shape, relay_shape),
        (vm, vm, pl.ANY),
        (from_left, from_right, own_a),
    )
    (own_b,) = call(
        lambda *refs: after_kernel(early // (SUB * NODES), *refs),
        "after",
        (((rows - early, wide), f32, vm),),
        (vm, vm, vm, pl.ANY),
        (weighted, numbers, points, relay_up),
    )
    corner_below = shift(relay_up, plan.lap)
    corner_above = shift(relay_down, -plan.lap)
    (advanced,) = call(
        lambda *refs: finish_kernel(plan, *refs),
        "finish",
        ((prognostic.shape, bf16, hbm),),
        (vm,) * 10,
        (fields, own_a, own_b, table, from_below, from_above, from_left, from_right, corner_below, corner_above),
        (vm(prognostic.shape, bf16), pltpu.SemaphoreType.DMA((4,))),
    )
    return advanced


def solution(mesh):
    placed = (
        P(None, AXES, None, None),
        P(None, AXES, None),
        P(AXES, None),
        P(AXES, None),
        P(AXES),
        P(AXES),
    )
    return jax.shard_map(
        local,
        mesh=mesh,
        in_specs=placed,
        out_specs=P(None, AXES, None, None),
        check_vma=False,
    )
```

```python
import math

import jax
import jax.numpy as jnp
import numpy as np
from jax import lax
from jax.experimental import pallas as pl
from jax.experimental.pallas import tpu as pltpu
from jax.sharding import PartitionSpec as P


STEP_SIZE = 0.1
AXES = ("face", "sub")
NODES = 16
SUB = 8
LANES = 128
MASS = 3 * LANES
MIB = 1024 * 1024
CARRIED = {0: (4, 7), 1: (6, 5)}
PASSED = ((4, 6), (7, 5))


def shift(value, steps):
    count = lax.axis_size(AXES)
    return lax.ppermute(value, AXES, [(d, (d + steps) % count) for d in range(count)])


def gll_tables():
    abscissa = np.array([-1.0, -math.sqrt(0.2), math.sqrt(0.2), 1.0])
    legendre = 0.5 * (5.0 * abscissa * abscissa * abscissa - 3.0 * abscissa)
    derivative = np.zeros((4, 4))
    for target in range(4):
        for source in range(4):
            if target != source:
                derivative[target, source] = legendre[target] / (
                    legendre[source] * (abscissa[target] - abscissa[source])
                )
    derivative[0, 0] = -3.0
    derivative[3, 3] = 3.0
    weights = np.array([1.0, 5.0, 5.0, 1.0]) / 6.0
    return (derivative, weights)


class Plan:
    def __init__(self, elements, links, lap):
        around = (links - 8) // 6
        short = 1
        while short * (around - short) < elements:
            short += 1
        side = 3 * short + 1
        top = 3 * (around - short) + 1
        first = [0]
        for count in (side, side, top, top, 1, 1, 1):
            first.append(first[-1] + count)
        self.offsets = (1, -1, lap, -lap, lap + 1, -lap - 1, lap - 1, 1 - lap)
        self.lap = lap
        self.tiles = top // SUB * SUB
        self.rest = top - self.tiles
        self.side_rows = -(-side // SUB) * SUB
        self.sides = 2 * self.tiles
        self.tail = self.sides + 2 * self.side_rows
        self.corner = self.tail + 2 * self.rest
        self.rows = -(-(self.corner + 4) // SUB) * SUB
        self.width = -(-self.rows // 256) * 256
        self.weight_rows = self.width // LANES
        self.spans = []
        for group in range(8):
            start = first[group]
            if group < 2:
                spans = ((start, self.sides + group * self.side_rows, side),)
            elif group < 4:
                spans = (
                    (start, (group - 2) * self.tiles, self.tiles),
                    (start + self.tiles, self.tail + (group - 2) * self.rest, self.rest),
                )
            else:
                spans = ((start, self.corner + group - 4, 1),)
            self.spans.append([span for span in spans if span[2]])

    def blocks(self, group):
        out = []
        place = 0
        for _, row, count in self.spans[group]:
            pitch = self.side_rows if group < 2 else count
            out.append((row, place, count, pitch))
            place += 3 * pitch
        for passed in CARRIED.get(group, ()):
            out.append((self.corner + passed - 4, place, 1, 1))
            place += 3
        return out

    def weight_row(self, group):
        _, place, _, pitch = self.blocks(group)[-1]
        return place + 3 * pitch

    def message_rows(self, group):
        return -(-(self.weight_row(group) + self.weight_rows) // SUB) * SUB

    def lanes(self, groups, index):
        at = iota((1, LANES), 1) + index * LANES
        mine = at < 0
        for group in groups:
            for _, row, count in self.spans[group]:
                mine = mine | ((at >= row) & (at < row + count))
        return mine


def iota(shape, axis):
    return lax.broadcasted_iota(jnp.int32, shape, axis)


def arranged(points_ref, plan):
    links = points_ref.shape[1]
    width = plan.width
    raw = points_ref[...].astype(jnp.float32)
    raw = jnp.concatenate([raw, jnp.full((1, width - links), -1.0, jnp.float32)], axis=1)
    raw = jnp.broadcast_to(raw, (SUB, width))
    lane = iota((SUB, width), 1)
    row = jnp.full((SUB, width), -1.0, jnp.float32)
    for spans in plan.spans:
        for source, target, count in spans:
            turned = pltpu.roll(raw, (target - source) % width, 1)
            row = jnp.where((lane >= target) & (lane < target + count), turned, row)
    return row[0:1]


def as_column(row, rows):
    width = row.shape[1]
    shape = (rows, width)
    return jnp.sum(jnp.where(iota(shape, 0) == iota(shape, 1), row, 0.0), axis=1, keepdims=True)


def as_row(column, width):
    shape = (column.shape[0], width)
    return jnp.sum(jnp.where(iota(shape, 0) == iota(shape, 1), column[:, :1], 0.0), axis=0, keepdims=True)


def point_rows(stack, first):
    elements = stack.shape[0]
    square = (LANES, LANES)
    spread = (iota(square, 1) // SUB + first == iota(square, 0)).astype(jnp.float32)
    wide = jnp.dot(stack, spread, precision=lax.Precision.HIGHEST, preferred_element_type=jnp.float32)
    mine = iota(wide.shape, 1) % SUB == iota(wide.shape, 0) % SUB
    return jnp.sum(jnp.where(mine, wide, 0.0).reshape(elements // SUB, SUB, LANES), axis=1)


def both_halves(mass):
    return mass + pltpu.roll(mass, LANES // 2, 1)


def split_lanes(mass):
    upper = mass.astype(jnp.bfloat16).astype(jnp.float32)
    return jnp.where(iota(mass.shape, 1) < LANES // 2, mass, mass - upper)


def derive(values, axis, scale):
    table, _ = gll_tables()
    out = [None] * NODES
    for other in range(4):
        spot = (lambda i: 4 * other + i) if axis == 1 else (lambda i: 4 * i + other)
        x0, x1, x2, x3 = (values[spot(i)] for i in range(4))
        diff_a = x0 - x3
        diff_b = x1 - x2
        even = (x0 + x3) - (x1 + x2)
        for i in (0, 1):
            factor = scale[other] * scale[i]
            p = even * np.float32(factor * 0.5 * (table[i, 0] + table[i, 3]))
            q = diff_a * np.float32(factor * 0.5 * (table[i, 0] - table[i, 3])) + diff_b * np.float32(
                factor * 0.5 * (table[i, 1] - table[i, 2])
            )
            out[spot(i)] = q + p
            out[spot(3 - i)] = q - p
    return out


def tendency_kernel(plan, *refs):
    prog, metric, cor, points, send, recv = refs[:6]
    fields, weighted, numbers, pts_v, recv_v = refs[6:11]
    messages = refs[11:15]
    met_v, cor_v, send_v, tile, mask, coefs, sems, chunk_sems = refs[15:]
    elements = fields.shape[1]
    groups = elements // SUB
    chunks = chunk_sems.shape[0]
    per = elements // chunks
    smalls = [
        pltpu.make_async_copy(source, target, sems.at[i])
        for i, (source, target) in enumerate(((points, pts_v), (send, send_v), (metric, met_v), (cor, cor_v)))
    ]
    for copy in smalls:
        copy.start()
    larges = [
        pltpu.make_async_copy(
            prog.at[:, pl.ds(i * per, per)], fields.at[:, pl.ds(i * per, per)], chunk_sems.at[i]
        )
        for i in range(chunks)
    ]
    for copy in larges:
        copy.start()
    later = pltpu.make_async_copy(recv, recv_v, sems.at[4])
    later.start()
    for copy in smalls:
        copy.wait()
    rows = plan.rows
    wanted = as_column(arranged(send_v, plan), rows)
    _, scale = gll_tables()
    a, b, e, g = (met_v[i] for i in range(4))
    node = iota(a.shape, 0)
    row_edge = (node // 4 == 0) | (node // 4 == 3)
    col_edge = (node % 4 == 0) | (node % 4 == 3)
    quad = jnp.where(row_edge, np.float32(scale[0]), np.float32(scale[1])) * jnp.where(
        col_edge, np.float32(scale[0]), np.float32(scale[1])
    )
    inv = 1.0 / (a * g - b * e)
    mass = quad * inv
    stack = (a * inv, b * inv, e * inv, g * inv, mass * cor_v[...], mass, pts_v[...].astype(jnp.float32))
    spare = LANES - len(stack) * NODES
    stack = jnp.concatenate(stack + (jnp.zeros((spare, elements), jnp.float32),), axis=0)
    coefs[...] = jnp.transpose(stack)
    numbers[...] = point_rows(coefs[...], 6 * NODES)
    for group in range(groups):
        mask[:, group * LANES : (group + 1) * LANES] = (
            jnp.broadcast_to(wanted, (rows, LANES)) == numbers[group : group + 1, :]
        ).astype(jnp.bfloat16)

    def body(group, carry):
        here = pl.ds(group * SUB, SUB)
        compact = coefs[here, :]

        def spread(which):
            lanes = range(which * NODES, (which + 1) * NODES)
            return [jnp.broadcast_to(compact[:, k : k + 1], (SUB, LANES)) for k in lanes]

        ca, cb, ce, cg, cf, cm = (spread(i) for i in range(6))
        for f in range(3):
            tile[f] = fields[f, here].astype(jnp.float32).reshape(SUB * NODES, LANES)
        u, v, h = ([tile[f, pl.ds(k, SUB, stride=NODES), :] for k in range(NODES)] for f in range(3))
        span = range(NODES)
        energy = [0.5 * (u[k] * u[k] + v[k] * v[k]) + h[k] for k in span]
        along = derive(energy, 1, scale)
        across = derive(energy, 0, scale)
        grad_one = [ca[k] * along[k] + ce[k] * across[k] for k in span]
        grad_two = [cb[k] * along[k] + cg[k] * across[k] for k in span]
        turn_two = derive([ca[k] * v[k] - cb[k] * u[k] for k in span], 1, scale)
        turn_one = derive([cg[k] * u[k] - ce[k] * v[k] for k in span], 0, scale)
        eta = [turn_two[k] - turn_one[k] + cf[k] for k in span]
        flow_one = derive([h[k] * (ca[k] * u[k] + cb[k] * v[k]) for k in span], 1, scale)
        flow_two = derive([h[k] * (ce[k] * u[k] + cg[k] * v[k]) for k in span], 0, scale)
        parts = (
            [eta[k] * v[k] - grad_one[k] for k in span],
            [-(eta[k] * u[k]) - grad_two[k] for k in span],
            [-(flow_one[k] + flow_two[k]) for k in span],
            [split_lanes(cm[k]) for k in span],
        )
        there = pl.ds(group * LANES, LANES)
        for f, part in enumerate(parts):
            weighted[there, f * LANES : (f + 1) * LANES] = jnp.concatenate(part, axis=0).astype(jnp.bfloat16)
        return carry

    step = groups // chunks
    for i in range(chunks):
        larges[i].wait()
        lax.fori_loop(i * step, (i + 1) * step, body, 0)
    later.wait()
    sums = jnp.dot(mask[...], weighted[...], preferred_element_type=jnp.float32)
    masses = as_row(both_halves(sums[:, MASS:]), plan.width)
    for group, ref in enumerate(messages):
        ref[ref.shape[0] - SUB :, :] = jnp.zeros((SUB, LANES), jnp.float32)
        for row, place, count, pitch in plan.blocks(group):
            span = pitch if pitch > count else count
            for f in range(3):
                ref[place + f * pitch : place + f * pitch + span, :] = sums[
                    row : row + span, f * LANES : (f + 1) * LANES
                ]
        for index in range(plan.weight_rows):
            mine = plan.lanes((group, *CARRIED.get(group, ())), index)
            at = plan.weight_row(group) + index
            ref[at : at + 1, :] = jnp.where(mine, masses[:, index * LANES : (index + 1) * LANES], 0.0)


def point_columns(points, group):
    return jnp.concatenate(
        [
            jnp.broadcast_to(points[:, e : e + 1], (NODES, LANES))
            for e in range(group * SUB, (group + 1) * SUB)
        ],
        axis=0,
    )


def local_sums(points, numbers, weighted, own):
    groups = weighted.shape[0] // LANES
    tall = SUB * NODES
    for i in range(own.shape[0] // tall):
        column = point_columns(points, i)
        same = jnp.concatenate(
            [(column == numbers[j : j + 1, :]).astype(jnp.bfloat16) for j in range(groups)], axis=1
        )
        own[i * tall : (i + 1) * tall, :] = jnp.dot(same, weighted[...], preferred_element_type=jnp.float32)


def local_kernel(plan, weighted, numbers, points, recv, own, table):
    landing = arranged(recv, plan)
    values = points[...].astype(jnp.float32)
    tall = SUB * NODES
    for group in range(numbers.shape[0]):
        column = point_columns(values, group)
        for i in range(0, plan.width, LANES):
            table[group * tall : (group + 1) * tall, i : i + LANES] = (
                column == landing[:, i : i + LANES]
            ).astype(jnp.bfloat16)
    local_sums(values, numbers, weighted, own)


def relay_kernel(plan, left, right, own, up, down):
    start = plan.weight_row(0)
    for i, ref in enumerate((up, down)):
        place = plan.blocks(0)[-2 + i][1]
        ref[0:3, :] = left[place : place + 3, :]
        ref[3:6, :] = right[place : place + 3, :]
        for index in range(plan.weight_rows):
            at = slice(start + index, start + index + 1)
            ref[6 + index : 7 + index, :] = jnp.where(
                plan.lanes(PASSED[i][:1], index), left[at, :], 0.0
            ) + jnp.where(plan.lanes(PASSED[i][1:], index), right[at, :], 0.0)


def finish_kernel(plan, fields, own, table, *refs):
    messages = refs[:4]
    relays = refs[4:6]
    out, held, landed, sems = refs[6:]
    width = plan.width
    landed[plan.tail :, :] = jnp.zeros((width - plan.tail, landed.shape[1]), jnp.float32)
    weights = []
    for index in range(plan.weight_rows):
        parts = [ref[6 + index : 7 + index, :] for ref in relays]
        for group, ref in enumerate(messages):
            at = plan.weight_row(group) + index
            row = ref[at : at + 1, :]
            parts.append(jnp.where(plan.lanes((group,), index), row, 0.0) if group < 2 else row)
        weights.append(sum(parts[1:], parts[0]))
    masses = as_column(jnp.concatenate(weights, axis=1), width)
    for group, ref in enumerate(messages):
        for row, place, count, pitch in plan.blocks(group)[: len(plan.spans[group])]:
            span = pitch if pitch > count else count
            for f in range(3):
                landed[row : row + span, f * LANES : (f + 1) * LANES] = ref[
                    place + f * pitch : place + f * pitch + span, :
                ]
    for passed, ref in zip(PASSED, relays):
        for i, group in enumerate(passed):
            row = plan.corner + group - 4
            for f in range(3):
                landed[row : row + 1, f * LANES : (f + 1) * LANES] = ref[3 * i + f : 3 * i + f + 1, :]
    landed[:, MASS:] = split_lanes(jnp.broadcast_to(masses, (width, LANES)))
    arrived = landed[...].astype(jnp.bfloat16)
    chunks = sems.shape[0]
    elements = fields.shape[1]
    per = elements // chunks
    copies = []
    for i in range(chunks):
        rows = slice(i * per * NODES, (i + 1) * per * NODES)
        here = slice(i * per, (i + 1) * per)
        total = own[rows, :] + jnp.dot(table[rows, :], arrived, preferred_element_type=jnp.float32)
        factor = np.float32(STEP_SIZE) / both_halves(total[:, MASS:])
        for f in range(3):
            moved = (total[:, f * LANES : (f + 1) * LANES] * factor).reshape(per, NODES, LANES)
            held[f, here] = (fields[f, here].astype(jnp.float32) + moved).astype(jnp.bfloat16)
        copy = pltpu.make_async_copy(
            held.at[:, pl.ds(i * per, per)], out.at[:, pl.ds(i * per, per)], sems.at[i]
        )
        copy.start()
        copies.append(copy)
    for copy in copies:
        copy.wait()


def in_hbm(value):
    return pltpu.with_memory_space_constraint(value, pltpu.HBM)


def call(kernel, outs, ins, args, scratch=(), limit=8 * MIB, flops=0):
    return pl.pallas_call(
        kernel,
        out_shape=[jax.ShapeDtypeStruct(shape, dtype) for shape, dtype, _ in outs],
        out_specs=[pl.BlockSpec(memory_space=space) for _, _, space in outs],
        in_specs=[pl.BlockSpec(memory_space=space) for space in ins],
        scratch_shapes=list(scratch),
        compiler_params=pltpu.CompilerParams(vmem_limit_bytes=limit),
        cost_estimate=pl.CostEstimate(flops=flops, bytes_accessed=0, transcendentals=0) if flops else None,
    )(*args)


def local(prognostic, metric, coriolis, node_point, send_point, recv_point):
    elements = prognostic.shape[1]
    levels = prognostic.shape[3]
    links = send_point.shape[0]
    plan = Plan(elements, links, 4 * lax.axis_size("sub"))
    rows = elements * NODES
    vm, hbm = pltpu.VMEM, pltpu.HBM
    f32, bf16 = jnp.float32, jnp.bfloat16
    send = send_point.reshape(1, links)
    recv = recv_point.reshape(1, links)
    metric = jnp.transpose(metric, (0, 2, 1))
    coriolis = jnp.transpose(coriolis)
    points = jnp.transpose(node_point)
    wide = 4 * levels
    sent = call(
        lambda *refs: tendency_kernel(plan, *refs),
        (
            (prognostic.shape, bf16, vm),
            ((rows, wide), bf16, vm),
            ((elements // SUB, LANES), f32, vm),
            (points.shape, jnp.int32, vm),
            (recv.shape, jnp.int32, vm),
        )
        + tuple(((plan.message_rows(group), LANES), f32, vm) for group in range(4)),
        (hbm,) * 6,
        tuple(in_hbm(x) for x in (prognostic, metric, coriolis, points, send, recv)),
        (
            vm(metric.shape, f32),
            vm(coriolis.shape, f32),
            vm(send.shape, jnp.int32),
            vm((3, SUB * NODES, levels), f32),
            vm((plan.rows, rows), bf16),
            vm((elements, LANES), f32),
            pltpu.SemaphoreType.DMA((5,)),
            pltpu.SemaphoreType.DMA((4,)),
        ),
    )
    fields, weighted, numbers, points, recv = sent[:5]
    landed = []
    for group in range(4):
        landed.append(shift(sent[5 + group], plan.offsets[group]))
    own, table = call(
        lambda *refs: local_kernel(plan, *refs),
        (((rows, wide), f32, vm), ((rows, plan.width), bf16, vm)),
        (vm,) * 4,
        (weighted, numbers, points, recv),
    )
    relays = call(
        lambda *refs: relay_kernel(plan, *refs),
        (((SUB, LANES), f32, vm),) * 2,
        (vm, vm, pl.ANY),
        (landed[0], landed[1], own),
    )
    passed = []
    for i, offset in enumerate((plan.lap, -plan.lap)):
        passed.append(shift(relays[i], offset))
    (advanced,) = call(
        lambda *refs: finish_kernel(plan, *refs),
        ((prognostic.shape, bf16, hbm),),
        (vm,) * 9,
        (fields, own, table, *landed, *passed),
        (
            vm(prognostic.shape, bf16),
            vm((plan.width, wide), f32),
            pltpu.SemaphoreType.DMA((4,)),
        ),
    )
    return advanced


def solution(mesh):
    placed = (
        P(None, AXES, None, None),
        P(None, AXES, None),
        P(AXES, None),
        P(AXES, None),
        P(AXES),
        P(AXES),
    )
    return jax.shard_map(
        local,
        mesh=mesh,
        in_specs=placed,
        out_specs=P(None, AXES, None, None),
        check_vma=False,
    )
```

```python
import math

import jax
import jax.numpy as jnp
import numpy as np
from jax import lax
from jax.experimental import pallas as pl
from jax.experimental.pallas import tpu as pltpu
from jax.sharding import PartitionSpec as P


STEP_SIZE = 0.1
AXES = ("face", "sub")
NODES = 16
SUB = 8
LANES = 128
MASS = 3 * LANES
MIB = 1024 * 1024
CARRIED = {0: (4, 7), 1: (6, 5)}
PASSED = ((4, 6), (7, 5))


def shift(value, steps):
    count = lax.axis_size(AXES)
    return lax.ppermute(value, AXES, [(d, (d + steps) % count) for d in range(count)])


def gll_tables():
    abscissa = np.array([-1.0, -math.sqrt(0.2), math.sqrt(0.2), 1.0])
    legendre = 0.5 * (5.0 * abscissa * abscissa * abscissa - 3.0 * abscissa)
    derivative = np.zeros((4, 4))
    for target in range(4):
        for source in range(4):
            if target != source:
                derivative[target, source] = legendre[target] / (
                    legendre[source] * (abscissa[target] - abscissa[source])
                )
    derivative[0, 0] = -3.0
    derivative[3, 3] = 3.0
    weights = np.array([1.0, 5.0, 5.0, 1.0]) / 6.0
    return (derivative, weights)


class Plan:
    def __init__(self, elements, links, lap):
        around = (links - 8) // 6
        short = 1
        while short * (around - short) < elements:
            short += 1
        side = 3 * short + 1
        top = 3 * (around - short) + 1
        first = [0]
        for count in (side, side, top, top, 1, 1, 1):
            first.append(first[-1] + count)
        self.offsets = (1, -1, lap, -lap, lap + 1, -lap - 1, lap - 1, 1 - lap)
        self.lap = lap
        self.tiles = top // SUB * SUB
        self.rest = top - self.tiles
        self.side_rows = -(-side // SUB) * SUB
        self.sides = 2 * self.tiles
        self.tail = self.sides + 2 * self.side_rows
        self.corner = self.tail + 2 * self.rest
        self.rows = -(-(self.corner + 4) // SUB) * SUB
        self.width = -(-self.rows // 256) * 256
        self.weight_rows = self.width // LANES
        self.spans = []
        for group in range(8):
            start = first[group]
            if group < 2:
                spans = ((start, self.sides + group * self.side_rows, side),)
            elif group < 4:
                spans = (
                    (start, (group - 2) * self.tiles, self.tiles),
                    (start + self.tiles, self.tail + (group - 2) * self.rest, self.rest),
                )
            else:
                spans = ((start, self.corner + group - 4, 1),)
            self.spans.append([span for span in spans if span[2]])

    def blocks(self, group):
        out = []
        place = 0
        for _, row, count in self.spans[group]:
            pitch = self.side_rows if group < 2 else count
            out.append((row, place, count, pitch))
            place += 3 * pitch
        for passed in CARRIED.get(group, ()):
            out.append((self.corner + passed - 4, place, 1, 1))
            place += 3
        return out

    def weight_row(self, group):
        _, place, _, pitch = self.blocks(group)[-1]
        return place + 3 * pitch

    def message_rows(self, group):
        return -(-(self.weight_row(group) + self.weight_rows) // SUB) * SUB

    def lanes(self, groups, index):
        at = iota((1, LANES), 1) + index * LANES
        mine = at < 0
        for group in groups:
            for _, row, count in self.spans[group]:
                mine = mine | ((at >= row) & (at < row + count))
        return mine


def iota(shape, axis):
    return lax.broadcasted_iota(jnp.int32, shape, axis)


def arranged(points_ref, plan):
    links = points_ref.shape[1]
    width = plan.width
    raw = points_ref[...].astype(jnp.float32)
    raw = jnp.concatenate([raw, jnp.full((1, width - links), -1.0, jnp.float32)], axis=1)
    raw = jnp.broadcast_to(raw, (SUB, width))
    lane = iota((SUB, width), 1)
    row = jnp.full((SUB, width), -1.0, jnp.float32)
    for spans in plan.spans:
        for source, target, count in spans:
            turned = pltpu.roll(raw, (target - source) % width, 1)
            row = jnp.where((lane >= target) & (lane < target + count), turned, row)
    return row[0:1]


def as_column(row, rows):
    width = row.shape[1]
    shape = (rows, width)
    return jnp.sum(jnp.where(iota(shape, 0) == iota(shape, 1), row, 0.0), axis=1, keepdims=True)


def as_row(column, width):
    shape = (column.shape[0], width)
    return jnp.sum(jnp.where(iota(shape, 0) == iota(shape, 1), column[:, :1], 0.0), axis=0, keepdims=True)


def point_rows(stack, first):
    elements = stack.shape[0]
    square = (LANES, LANES)
    spread = (iota(square, 1) // SUB + first == iota(square, 0)).astype(jnp.float32)
    wide = jnp.dot(stack, spread, precision=lax.Precision.HIGHEST, preferred_element_type=jnp.float32)
    mine = iota(wide.shape, 1) % SUB == iota(wide.shape, 0) % SUB
    return jnp.sum(jnp.where(mine, wide, 0.0).reshape(elements // SUB, SUB, LANES), axis=1)


def both_halves(mass):
    return mass + pltpu.roll(mass, LANES // 2, 1)


def split_lanes(mass):
    upper = mass.astype(jnp.bfloat16).astype(jnp.float32)
    return jnp.where(iota(mass.shape, 1) < LANES // 2, mass, mass - upper)


def derive(values, axis, scale, sign=1.0):
    table, _ = gll_tables()
    out = [None] * NODES
    for other in range(4):
        spot = (lambda i: 4 * other + i) if axis == 1 else (lambda i: 4 * i + other)
        x0, x1, x2, x3 = (values[spot(i)] for i in range(4))
        diff_a = x0 - x3
        diff_b = x1 - x2
        even = (x0 + x3) - (x1 + x2)
        for i in (0, 1):
            factor = sign * scale[other] * scale[i]
            p = even * np.float32(factor * 0.5 * (table[i, 0] + table[i, 3]))
            q = diff_a * np.float32(factor * 0.5 * (table[i, 0] - table[i, 3])) + diff_b * np.float32(
                factor * 0.5 * (table[i, 1] - table[i, 2])
            )
            out[spot(i)] = q + p
            out[spot(3 - i)] = q - p
    return out


def tendency_kernel(plan, *refs):
    prog, metric, cor, points, send, recv = refs[:6]
    fields, weighted, numbers, pts_v, recv_v = refs[6:11]
    messages = refs[11:15]
    met_v, cor_v, send_v, tile, mask, total, coefs, sems, chunk_sems = refs[15:]
    elements = fields.shape[1]
    groups = elements // SUB
    chunks = chunk_sems.shape[0]
    per = elements // chunks
    smalls = [
        pltpu.make_async_copy(source, target, sems.at[i])
        for i, (source, target) in enumerate(((points, pts_v), (send, send_v), (metric, met_v), (cor, cor_v)))
    ]
    for copy in smalls:
        copy.start()
    larges = [
        pltpu.make_async_copy(
            prog.at[:, pl.ds(i * per, per)], fields.at[:, pl.ds(i * per, per)], chunk_sems.at[i]
        )
        for i in range(chunks)
    ]
    larges[0].start()
    later = pltpu.make_async_copy(recv, recv_v, sems.at[4])
    later.start()
    for copy in smalls:
        copy.wait()
    for copy in larges[1:]:
        copy.start()
    rows = plan.rows
    wanted = as_column(arranged(send_v, plan), rows)
    _, scale = gll_tables()
    a, b, e, g = (met_v[i] for i in range(4))
    node = iota(a.shape, 0)
    row_edge = (node // 4 == 0) | (node // 4 == 3)
    col_edge = (node % 4 == 0) | (node % 4 == 3)
    quad = jnp.where(row_edge, np.float32(scale[0]), np.float32(scale[1])) * jnp.where(
        col_edge, np.float32(scale[0]), np.float32(scale[1])
    )
    inv = 1.0 / (a * g - b * e)
    mass = quad * inv
    upper = mass.astype(jnp.bfloat16).astype(jnp.float32)
    stack = (a * inv, b * inv, e * inv, g * inv, mass * cor_v[...], upper, mass - upper, pts_v[...].astype(jnp.float32))
    stack = jnp.transpose(jnp.concatenate(stack, axis=0))
    numbers[...] = point_rows(stack, 7 * NODES)
    square = (LANES, LANES)
    kind = iota(square, 0) // NODES
    half = (iota(square, 1) >= LANES // 2).astype(jnp.int32)
    lift = [(kind == i).astype(jnp.bfloat16) for i in range(5)]
    fine = jnp.concatenate(lift + [jnp.zeros(square, jnp.bfloat16)], axis=1)
    lift = jnp.concatenate([jnp.concatenate(lift + [(kind == 5 + half).astype(jnp.bfloat16)], axis=1), fine], axis=0)
    coarse = stack.astype(jnp.bfloat16).astype(jnp.float32)
    slot = iota((SUB, LANES), 1) % NODES
    for group in range(groups):
        here = slice(group * SUB, (group + 1) * SUB)
        picked = jnp.concatenate(
            [
                jnp.concatenate([jnp.where(slot == k, part[here], 0.0) for k in range(NODES)], axis=0)
                for part in (coarse, stack - coarse)
            ],
            axis=1,
        ).astype(jnp.bfloat16)
        there = slice(group * LANES, (group + 1) * LANES)
        wide = jnp.dot(picked, lift, preferred_element_type=jnp.float32)
        for i in range(5):
            coefs[i, there, :] = wide[:, i * LANES : (i + 1) * LANES]
        weighted[there, MASS:] = wide[:, 5 * LANES :].astype(jnp.bfloat16)
    for group in range(groups):
        mask[:, group * LANES : (group + 1) * LANES] = (
            jnp.broadcast_to(wanted, (rows, LANES)) == numbers[group : group + 1, :]
        ).astype(jnp.bfloat16)

    def body(group):
        ca, cb, ce, cg, cf = (
            [coefs[i, (group * NODES + k) * SUB : (group * NODES + k + 1) * SUB, :] for k in range(NODES)]
            for i in range(5)
        )
        u, v, h = ([tile[group, f, k * SUB : (k + 1) * SUB, :] for k in range(NODES)] for f in range(3))
        span = range(NODES)
        energy = [0.5 * (u[k] * u[k] + v[k] * v[k]) + h[k] for k in span]
        along = derive(energy, 1, scale, -1.0)
        across = derive(energy, 0, scale, -1.0)
        grad_one = [ca[k] * along[k] + ce[k] * across[k] for k in span]
        grad_two = [cb[k] * along[k] + cg[k] * across[k] for k in span]
        turn_two = derive([ca[k] * v[k] - cb[k] * u[k] for k in span], 1, scale)
        turn_one = derive([cg[k] * u[k] - ce[k] * v[k] for k in span], 0, scale)
        eta = [turn_two[k] - turn_one[k] + cf[k] for k in span]
        flow_one = derive([h[k] * (ca[k] * u[k] + cb[k] * v[k]) for k in span], 1, scale, -1.0)
        flow_two = derive([h[k] * (ce[k] * u[k] + cg[k] * v[k]) for k in span], 0, scale, -1.0)
        parts = (
            [eta[k] * v[k] + grad_one[k] for k in span],
            [grad_two[k] - eta[k] * u[k] for k in span],
            [flow_one[k] + flow_two[k] for k in span],
        )
        there = slice(group * LANES, (group + 1) * LANES)
        for f, part in enumerate(parts):
            weighted[there, f * LANES : (f + 1) * LANES] = jnp.concatenate(part, axis=0).astype(jnp.bfloat16)

    step = groups // chunks
    turn = (
        iota(square, 1) == iota(square, 0) % SUB * NODES + iota(square, 0) // SUB
    ).astype(jnp.bfloat16)

    def reorder(i):
        larges[i].wait()
        for group in range(i * step, (i + 1) * step):
            here = slice(group * SUB, (group + 1) * SUB)
            for f in range(3):
                tile[group, f] = jnp.dot(
                    turn, fields[f, here].reshape(SUB * NODES, LANES), preferred_element_type=jnp.float32
                )

    def gather(i):
        span = slice(i * step * LANES, (i + 1) * step * LANES)
        part = jnp.dot(mask[:, span], weighted[span, :], preferred_element_type=jnp.float32)
        total[...] = part if i == 0 else total[...] + part

    reorder(0)
    for i in range(chunks):
        if i + 1 < chunks:
            reorder(i + 1)
        for group in range(i * step, (i + 1) * step):
            body(group)
        if i:
            gather(i - 1)
    gather(chunks - 1)
    later.wait()
    sums = total[...]
    masses = as_row(both_halves(sums[:, MASS:]), plan.width)
    for group, ref in enumerate(messages):
        ref[ref.shape[0] - SUB :, :] = jnp.zeros((SUB, LANES), jnp.float32)
        for row, place, count, pitch in plan.blocks(group):
            span = pitch if pitch > count else count
            for f in range(3):
                ref[place + f * pitch : place + f * pitch + span, :] = sums[
                    row : row + span, f * LANES : (f + 1) * LANES
                ]
        for index in range(plan.weight_rows):
            mine = plan.lanes((group, *CARRIED.get(group, ())), index)
            at = plan.weight_row(group) + index
            ref[at : at + 1, :] = jnp.where(mine, masses[:, index * LANES : (index + 1) * LANES], 0.0)


def point_columns(points, group):
    return jnp.concatenate(
        [
            jnp.broadcast_to(points[:, e : e + 1], (NODES, LANES))
            for e in range(group * SUB, (group + 1) * SUB)
        ],
        axis=0,
    )


def local_sums(points, numbers, weighted, own):
    groups = weighted.shape[0] // LANES
    tall = SUB * NODES
    for i in range(own.shape[0] // tall):
        column = point_columns(points, i)
        same = jnp.concatenate(
            [(column == numbers[j : j + 1, :]).astype(jnp.bfloat16) for j in range(groups)], axis=1
        )
        own[i * tall : (i + 1) * tall, :] = jnp.dot(same, weighted[...], preferred_element_type=jnp.float32)


def local_kernel(plan, weighted, numbers, points, recv, own, table):
    landing = arranged(recv, plan)
    values = points[...].astype(jnp.float32)
    tall = SUB * NODES
    for group in range(numbers.shape[0]):
        column = point_columns(values, group)
        for i in range(0, plan.width, LANES):
            table[group * tall : (group + 1) * tall, i : i + LANES] = (
                column == landing[:, i : i + LANES]
            ).astype(jnp.bfloat16)
    local_sums(values, numbers, weighted, own)


def relay_kernel(plan, left, right, own, up, down):
    start = plan.weight_row(0)
    for i, ref in enumerate((up, down)):
        place = plan.blocks(0)[-2 + i][1]
        ref[0:3, :] = left[place : place + 3, :]
        ref[3:6, :] = right[place : place + 3, :]
        for index in range(plan.weight_rows):
            at = slice(start + index, start + index + 1)
            ref[6 + index : 7 + index, :] = jnp.where(
                plan.lanes(PASSED[i][:1], index), left[at, :], 0.0
            ) + jnp.where(plan.lanes(PASSED[i][1:], index), right[at, :], 0.0)


def finish_kernel(plan, fields, own, table, *refs):
    messages = refs[:4]
    relays = refs[4:6]
    out, held, landed, sems = refs[6:]
    width = plan.width
    landed[plan.tail :, :] = jnp.zeros((width - plan.tail, landed.shape[1]), jnp.float32)
    weights = []
    for index in range(plan.weight_rows):
        parts = [ref[6 + index : 7 + index, :] for ref in relays]
        for group, ref in enumerate(messages):
            at = plan.weight_row(group) + index
            row = ref[at : at + 1, :]
            parts.append(jnp.where(plan.lanes((group,), index), row, 0.0) if group < 2 else row)
        weights.append(sum(parts[1:], parts[0]))
    masses = as_column(jnp.concatenate(weights, axis=1), width)
    for group, ref in enumerate(messages):
        for row, place, count, pitch in plan.blocks(group)[: len(plan.spans[group])]:
            span = pitch if pitch > count else count
            for f in range(3):
                landed[row : row + span, f * LANES : (f + 1) * LANES] = ref[
                    place + f * pitch : place + f * pitch + span, :
                ]
    for passed, ref in zip(PASSED, relays):
        for i, group in enumerate(passed):
            row = plan.corner + group - 4
            for f in range(3):
                landed[row : row + 1, f * LANES : (f + 1) * LANES] = ref[3 * i + f : 3 * i + f + 1, :]
    landed[:, MASS:] = split_lanes(jnp.broadcast_to(masses, (width, LANES)))
    arrived = landed[...].astype(jnp.bfloat16)
    chunks = sems.shape[0]
    elements = fields.shape[1]
    per = elements // chunks
    copies = []
    for i in range(chunks):
        rows = slice(i * per * NODES, (i + 1) * per * NODES)
        here = slice(i * per, (i + 1) * per)
        total = own[rows, :] + jnp.dot(table[rows, :], arrived, preferred_element_type=jnp.float32)
        factor = np.float32(STEP_SIZE) / both_halves(total[:, MASS:])
        for f in range(3):
            moved = (total[:, f * LANES : (f + 1) * LANES] * factor).reshape(per, NODES, LANES)
            held[f, here] = (fields[f, here].astype(jnp.float32) + moved).astype(jnp.bfloat16)
        copy = pltpu.make_async_copy(
            held.at[:, pl.ds(i * per, per)], out.at[:, pl.ds(i * per, per)], sems.at[i]
        )
        copy.start()
        copies.append(copy)
    for copy in copies:
        copy.wait()


def in_hbm(value):
    return pltpu.with_memory_space_constraint(value, pltpu.HBM)


def call(kernel, outs, ins, args, scratch=(), limit=8 * MIB, flops=0):
    return pl.pallas_call(
        kernel,
        out_shape=[jax.ShapeDtypeStruct(shape, dtype) for shape, dtype, _ in outs],
        out_specs=[pl.BlockSpec(memory_space=space) for _, _, space in outs],
        in_specs=[pl.BlockSpec(memory_space=space) for space in ins],
        scratch_shapes=list(scratch),
        compiler_params=pltpu.CompilerParams(vmem_limit_bytes=limit),
        cost_estimate=pl.CostEstimate(flops=flops, bytes_accessed=0, transcendentals=0) if flops else None,
    )(*args)


def local(prognostic, metric, coriolis, node_point, send_point, recv_point):
    elements = prognostic.shape[1]
    levels = prognostic.shape[3]
    links = send_point.shape[0]
    plan = Plan(elements, links, 4 * lax.axis_size("sub"))
    rows = elements * NODES
    vm, hbm = pltpu.VMEM, pltpu.HBM
    f32, bf16 = jnp.float32, jnp.bfloat16
    send = send_point.reshape(1, links)
    recv = recv_point.reshape(1, links)
    metric = jnp.transpose(metric, (0, 2, 1))
    coriolis = jnp.transpose(coriolis)
    points = jnp.transpose(node_point)
    wide = 4 * levels
    sent = call(
        lambda *refs: tendency_kernel(plan, *refs),
        (
            (prognostic.shape, bf16, vm),
            ((rows, wide), bf16, vm),
            ((elements // SUB, LANES), f32, vm),
            (points.shape, jnp.int32, vm),
            (recv.shape, jnp.int32, vm),
        )
        + tuple(((plan.message_rows(group), LANES), f32, vm) for group in range(4)),
        (hbm,) * 6,
        tuple(in_hbm(x) for x in (prognostic, metric, coriolis, points, send, recv)),
        (
            vm(metric.shape, f32),
            vm(coriolis.shape, f32),
            vm(send.shape, jnp.int32),
            vm((elements // SUB, 3, SUB * NODES, levels), f32),
            vm((plan.rows, rows), bf16),
            vm((plan.rows, wide), f32),
            vm((5, rows, LANES), f32),
            pltpu.SemaphoreType.DMA((5,)),
            pltpu.SemaphoreType.DMA((4,)),
        ),
    )
    fields, weighted, numbers, points, recv = sent[:5]
    landed = []
    for group in range(4):
        landed.append(shift(sent[5 + group], plan.offsets[group]))
    own, table = call(
        lambda *refs: local_kernel(plan, *refs),
        (((rows, wide), f32, vm), ((rows, plan.width), bf16, vm)),
        (vm,) * 4,
        (weighted, numbers, points, recv),
    )
    relays = call(
        lambda *refs: relay_kernel(plan, *refs),
        (((SUB, LANES), f32, vm),) * 2,
        (vm, vm, pl.ANY),
        (landed[0], landed[1], own),
    )
    passed = []
    for i, offset in enumerate((plan.lap, -plan.lap)):
        passed.append(shift(relays[i], offset))
    (advanced,) = call(
        lambda *refs: finish_kernel(plan, *refs),
        ((prognostic.shape, bf16, hbm),),
        (vm,) * 9,
        (fields, own, table, *landed, *passed),
        (
            vm(prognostic.shape, bf16),
            vm((plan.width, wide), f32),
            pltpu.SemaphoreType.DMA((4,)),
        ),
    )
    return advanced


def solution(mesh):
    placed = (
        P(None, AXES, None, None),
        P(None, AXES, None),
        P(AXES, None),
        P(AXES, None),
        P(AXES),
        P(AXES),
    )
    return jax.shard_map(
        local,
        mesh=mesh,
        in_specs=placed,
        out_specs=P(None, AXES, None, None),
        check_vma=False,
    )
```

```python
import math

import jax
import jax.numpy as jnp
import numpy as np
from jax import lax
from jax.experimental import pallas as pl
from jax.experimental.pallas import tpu as pltpu
from jax.sharding import PartitionSpec as P


STEP_SIZE = 0.1
AXES = ("face", "sub")
NODES = 16
SUB = 8
LANES = 128
MASS = 3 * LANES
MIB = 1024 * 1024
CARRIED = {0: (4, 7), 1: (6, 5)}
PASSED = ((4, 6), (7, 5))


def shift(value, steps):
    count = lax.axis_size(AXES)
    return lax.ppermute(value, AXES, [(d, (d + steps) % count) for d in range(count)])


def gll_tables():
    abscissa = np.array([-1.0, -math.sqrt(0.2), math.sqrt(0.2), 1.0])
    legendre = 0.5 * (5.0 * abscissa * abscissa * abscissa - 3.0 * abscissa)
    derivative = np.zeros((4, 4))
    for target in range(4):
        for source in range(4):
            if target != source:
                derivative[target, source] = legendre[target] / (
                    legendre[source] * (abscissa[target] - abscissa[source])
                )
    derivative[0, 0] = -3.0
    derivative[3, 3] = 3.0
    weights = np.array([1.0, 5.0, 5.0, 1.0]) / 6.0
    return (derivative, weights)


class Plan:
    def __init__(self, elements, links, lap):
        around = (links - 8) // 6
        short = 1
        while short * (around - short) < elements:
            short += 1
        side = 3 * short + 1
        top = 3 * (around - short) + 1
        first = [0]
        for count in (side, side, top, top, 1, 1, 1):
            first.append(first[-1] + count)
        self.offsets = (1, -1, lap, -lap, lap + 1, -lap - 1, lap - 1, 1 - lap)
        self.lap = lap
        self.tiles = top // SUB * SUB
        self.rest = top - self.tiles
        self.side_rows = -(-side // SUB) * SUB
        self.sides = 2 * self.tiles
        self.tail = self.sides + 2 * self.side_rows
        self.corner = self.tail + 2 * self.rest
        self.rows = -(-(self.corner + 4) // SUB) * SUB
        self.width = -(-self.rows // 256) * 256
        self.weight_rows = self.width // LANES
        self.spans = []
        for group in range(8):
            start = first[group]
            if group < 2:
                spans = ((start, self.sides + group * self.side_rows, side),)
            elif group < 4:
                spans = (
                    (start, (group - 2) * self.tiles, self.tiles),
                    (start + self.tiles, self.tail + (group - 2) * self.rest, self.rest),
                )
            else:
                spans = ((start, self.corner + group - 4, 1),)
            self.spans.append([span for span in spans if span[2]])

    def blocks(self, group):
        out = []
        place = 0
        for _, row, count in self.spans[group]:
            pitch = self.side_rows if group < 2 else count
            out.append((row, place, count, pitch))
            place += 3 * pitch
        for passed in CARRIED.get(group, ()):
            out.append((self.corner + passed - 4, place, 1, 1))
            place += 3
        return out

    def weight_row(self, group):
        _, place, _, pitch = self.blocks(group)[-1]
        return place + 3 * pitch

    def message_rows(self, group):
        return -(-(self.weight_row(group) + self.weight_rows) // SUB) * SUB

    def lanes(self, groups, index):
        at = iota((1, LANES), 1) + index * LANES
        mine = at < 0
        for group in groups:
            for _, row, count in self.spans[group]:
                mine = mine | ((at >= row) & (at < row + count))
        return mine


def iota(shape, axis):
    return lax.broadcasted_iota(jnp.int32, shape, axis)


def arranged(points_ref, plan):
    links = points_ref.shape[1]
    width = plan.width
    raw = points_ref[...].astype(jnp.float32)
    raw = jnp.concatenate([raw, jnp.full((1, width - links), -1.0, jnp.float32)], axis=1)
    raw = jnp.broadcast_to(raw, (SUB, width))
    lane = iota((SUB, width), 1)
    row = jnp.full((SUB, width), -1.0, jnp.float32)
    for spans in plan.spans:
        for source, target, count in spans:
            turned = pltpu.roll(raw, (target - source) % width, 1)
            row = jnp.where((lane >= target) & (lane < target + count), turned, row)
    return row[0:1]


def as_column(row, rows):
    width = row.shape[1]
    shape = (rows, width)
    return jnp.sum(jnp.where(iota(shape, 0) == iota(shape, 1), row, 0.0), axis=1, keepdims=True)


def as_row(column, width):
    shape = (column.shape[0], width)
    return jnp.sum(jnp.where(iota(shape, 0) == iota(shape, 1), column[:, :1], 0.0), axis=0, keepdims=True)


def point_rows(stack, first):
    elements = stack.shape[0]
    square = (LANES, LANES)
    spread = (iota(square, 1) // SUB + first == iota(square, 0)).astype(jnp.float32)
    wide = jnp.dot(stack, spread, precision=lax.Precision.HIGHEST, preferred_element_type=jnp.float32)
    mine = iota(wide.shape, 1) % SUB == iota(wide.shape, 0) % SUB
    return jnp.sum(jnp.where(mine, wide, 0.0).reshape(elements // SUB, SUB, LANES), axis=1)


def both_halves(mass):
    return mass + pltpu.roll(mass, LANES // 2, 1)


def split_lanes(mass):
    upper = mass.astype(jnp.bfloat16).astype(jnp.float32)
    return jnp.where(iota(mass.shape, 1) < LANES // 2, mass, mass - upper)


def derive(values, axis, scale, sign=1.0):
    table, _ = gll_tables()
    out = [None] * NODES
    for other in range(4):
        spot = (lambda i: 4 * other + i) if axis == 1 else (lambda i: 4 * i + other)
        x0, x1, x2, x3 = (values[spot(i)] for i in range(4))
        diff_a = x0 - x3
        diff_b = x1 - x2
        even = (x0 + x3) - (x1 + x2)
        for i in (0, 1):
            factor = sign * scale[other] * scale[i]
            p = even * np.float32(factor * 0.5 * (table[i, 0] + table[i, 3]))
            q = diff_a * np.float32(factor * 0.5 * (table[i, 0] - table[i, 3])) + diff_b * np.float32(
                factor * 0.5 * (table[i, 1] - table[i, 2])
            )
            out[spot(i)] = q + p
            out[spot(3 - i)] = q - p
    return out


def tendency_kernel(plan, *refs):
    prog, metric, cor, points, send, recv = refs[:6]
    fields, weighted, numbers, pts_v, recv_v = refs[6:11]
    messages = refs[11:15]
    met_v, cor_v, send_v, tile, mask, total, coefs, sems, chunk_sems = refs[15:]
    elements = fields.shape[1]
    groups = elements // SUB
    chunks = chunk_sems.shape[0]
    per = elements // chunks
    smalls = [
        pltpu.make_async_copy(source, target, sems.at[i])
        for i, (source, target) in enumerate(((points, pts_v), (send, send_v), (metric, met_v), (cor, cor_v)))
    ]
    for copy in smalls:
        copy.start()
    larges = [
        pltpu.make_async_copy(
            prog.at[:, pl.ds(i * per, per)], fields.at[:, pl.ds(i * per, per)], chunk_sems.at[i]
        )
        for i in range(chunks)
    ]
    larges[0].start()
    later = pltpu.make_async_copy(recv, recv_v, sems.at[4])
    later.start()
    for copy in smalls:
        copy.wait()
    for copy in larges[1:]:
        copy.start()
    rows = plan.rows
    wanted = as_column(arranged(send_v, plan), rows)
    _, scale = gll_tables()
    a, b, e, g = (met_v[i] for i in range(4))
    node = iota(a.shape, 0)
    row_edge = (node // 4 == 0) | (node // 4 == 3)
    col_edge = (node % 4 == 0) | (node % 4 == 3)
    quad = jnp.where(row_edge, np.float32(scale[0]), np.float32(scale[1])) * jnp.where(
        col_edge, np.float32(scale[0]), np.float32(scale[1])
    )
    inv = 1.0 / (a * g - b * e)
    mass = quad * inv
    upper = mass.astype(jnp.bfloat16).astype(jnp.float32)
    stack = (a * inv, b * inv, e * inv, g * inv, mass * cor_v[...], upper, mass - upper, pts_v[...].astype(jnp.float32))
    stack = jnp.transpose(jnp.concatenate(stack, axis=0))
    numbers[...] = point_rows(stack, 7 * NODES)
    square = (LANES, LANES)
    kind = iota(square, 0) // NODES
    half = (iota(square, 1) >= LANES // 2).astype(jnp.int32)
    lift = [(kind == i).astype(jnp.bfloat16) for i in range(5)]
    fine = jnp.concatenate(lift + [jnp.zeros(square, jnp.bfloat16)], axis=1)
    lift = jnp.concatenate([jnp.concatenate(lift + [(kind == 5 + half).astype(jnp.bfloat16)], axis=1), fine], axis=0)
    coarse = stack.astype(jnp.bfloat16).astype(jnp.float32)
    slot = iota((SUB, LANES), 1) % NODES
    for group in range(groups):
        here = slice(group * SUB, (group + 1) * SUB)
        picked = jnp.concatenate(
            [
                jnp.concatenate([jnp.where(slot == k, part[here], 0.0) for k in range(NODES)], axis=0)
                for part in (coarse, stack - coarse)
            ],
            axis=1,
        ).astype(jnp.bfloat16)
        there = slice(group * LANES, (group + 1) * LANES)
        wide = jnp.dot(picked, lift, preferred_element_type=jnp.float32)
        for i in range(5):
            coefs[i, there, :] = wide[:, i * LANES : (i + 1) * LANES]
        weighted[there, MASS:] = wide[:, 5 * LANES :].astype(jnp.bfloat16)
    for group in range(groups):
        mask[:, group * LANES : (group + 1) * LANES] = (
            jnp.broadcast_to(wanted, (rows, LANES)) == numbers[group : group + 1, :]
        ).astype(jnp.bfloat16)

    def body(group):
        ca, cb, ce, cg, cf = (
            [coefs[i, (group * NODES + k) * SUB : (group * NODES + k + 1) * SUB, :] for k in range(NODES)]
            for i in range(5)
        )
        u, v, h = ([tile[group, f, k * SUB : (k + 1) * SUB, :] for k in range(NODES)] for f in range(3))
        span = range(NODES)
        energy = [0.5 * (u[k] * u[k] + v[k] * v[k]) + h[k] for k in span]
        along = derive(energy, 1, scale, -1.0)
        across = derive(energy, 0, scale, -1.0)
        grad_one = [ca[k] * along[k] + ce[k] * across[k] for k in span]
        grad_two = [cb[k] * along[k] + cg[k] * across[k] for k in span]
        turn_two = derive([ca[k] * v[k] - cb[k] * u[k] for k in span], 1, scale)
        turn_one = derive([cg[k] * u[k] - ce[k] * v[k] for k in span], 0, scale)
        eta = [turn_two[k] - turn_one[k] + cf[k] for k in span]
        flow_one = derive([h[k] * (ca[k] * u[k] + cb[k] * v[k]) for k in span], 1, scale, -1.0)
        flow_two = derive([h[k] * (ce[k] * u[k] + cg[k] * v[k]) for k in span], 0, scale, -1.0)
        parts = (
            [eta[k] * v[k] + grad_one[k] for k in span],
            [grad_two[k] - eta[k] * u[k] for k in span],
            [flow_one[k] + flow_two[k] for k in span],
        )
        there = slice(group * LANES, (group + 1) * LANES)
        for f, part in enumerate(parts):
            weighted[there, f * LANES : (f + 1) * LANES] = jnp.concatenate(part, axis=0).astype(jnp.bfloat16)

    step = groups // chunks
    turn = (
        iota(square, 1) == iota(square, 0) % SUB * NODES + iota(square, 0) // SUB
    ).astype(jnp.bfloat16)

    def reorder(i):
        larges[i].wait()
        for group in range(i * step, (i + 1) * step):
            here = slice(group * SUB, (group + 1) * SUB)
            for f in range(3):
                tile[group, f] = jnp.dot(
                    turn, fields[f, here].reshape(SUB * NODES, LANES), preferred_element_type=jnp.float32
                )

    def gather(i):
        span = slice(i * step * LANES, (i + 1) * step * LANES)
        part = jnp.dot(mask[:, span], weighted[span, :], preferred_element_type=jnp.float32)
        total[...] = part if i == 0 else total[...] + part

    reorder(0)
    for i in range(chunks):
        if i + 1 < chunks:
            reorder(i + 1)
        for group in range(i * step, (i + 1) * step):
            body(group)
        if i:
            gather(i - 1)
    gather(chunks - 1)
    later.wait()
    sums = total[...]
    masses = as_row(both_halves(sums[:, MASS:]), plan.width)
    for group, ref in enumerate(messages):
        ref[ref.shape[0] - SUB :, :] = jnp.zeros((SUB, LANES), jnp.float32)
        for row, place, count, pitch in plan.blocks(group):
            span = pitch if pitch > count else count
            for f in range(3):
                ref[place + f * pitch : place + f * pitch + span, :] = sums[
                    row : row + span, f * LANES : (f + 1) * LANES
                ]
        for index in range(plan.weight_rows):
            mine = plan.lanes((group, *CARRIED.get(group, ())), index)
            at = plan.weight_row(group) + index
            ref[at : at + 1, :] = jnp.where(mine, masses[:, index * LANES : (index + 1) * LANES], 0.0)


def point_columns(points, group):
    return jnp.concatenate(
        [
            jnp.broadcast_to(points[:, e : e + 1], (NODES, LANES))
            for e in range(group * SUB, (group + 1) * SUB)
        ],
        axis=0,
    )


def local_sums(points, numbers, weighted, own):
    groups = weighted.shape[0] // LANES
    tall = SUB * NODES
    for i in range(own.shape[0] // tall):
        column = point_columns(points, i)
        same = jnp.concatenate(
            [(column == numbers[j : j + 1, :]).astype(jnp.bfloat16) for j in range(groups)], axis=1
        )
        own[i * tall : (i + 1) * tall, :] = jnp.dot(same, weighted[...], preferred_element_type=jnp.float32)


def local_kernel(plan, weighted, numbers, points, recv, own, table):
    landing = arranged(recv, plan)
    values = points[...].astype(jnp.float32)
    tall = SUB * NODES
    for group in range(numbers.shape[0]):
        column = point_columns(values, group)
        for i in range(0, plan.width, LANES):
            table[group * tall : (group + 1) * tall, i : i + LANES] = (
                column == landing[:, i : i + LANES]
            ).astype(jnp.bfloat16)
    local_sums(values, numbers, weighted, own)


def relay_kernel(plan, left, right, up, down):
    start = plan.weight_row(0)
    for i, ref in enumerate((up, down)):
        place = plan.blocks(0)[-2 + i][1]
        ref[0:3, :] = left[place : place + 3, :]
        ref[3:6, :] = right[place : place + 3, :]
        for index in range(plan.weight_rows):
            at = slice(start + index, start + index + 1)
            ref[6 + index : 7 + index, :] = jnp.where(
                plan.lanes(PASSED[i][:1], index), left[at, :], 0.0
            ) + jnp.where(plan.lanes(PASSED[i][1:], index), right[at, :], 0.0)


def finish_kernel(plan, fields, own, table, *refs):
    messages = refs[:4]
    relays = refs[4:6]
    out, held, landed, sems = refs[6:]
    width = plan.width
    landed[plan.tail :, :] = jnp.zeros((width - plan.tail, landed.shape[1]), jnp.float32)
    weights = []
    for index in range(plan.weight_rows):
        parts = [ref[6 + index : 7 + index, :] for ref in relays]
        for group, ref in enumerate(messages):
            at = plan.weight_row(group) + index
            row = ref[at : at + 1, :]
            parts.append(jnp.where(plan.lanes((group,), index), row, 0.0) if group < 2 else row)
        weights.append(sum(parts[1:], parts[0]))
    masses = as_column(jnp.concatenate(weights, axis=1), width)
    for group, ref in enumerate(messages):
        for row, place, count, pitch in plan.blocks(group)[: len(plan.spans[group])]:
            span = pitch if pitch > count else count
            for f in range(3):
                landed[row : row + span, f * LANES : (f + 1) * LANES] = ref[
                    place + f * pitch : place + f * pitch + span, :
                ]
    for passed, ref in zip(PASSED, relays):
        for i, group in enumerate(passed):
            row = plan.corner + group - 4
            for f in range(3):
                landed[row : row + 1, f * LANES : (f + 1) * LANES] = ref[3 * i + f : 3 * i + f + 1, :]
    landed[:, MASS:] = split_lanes(jnp.broadcast_to(masses, (width, LANES)))
    arrived = landed[...].astype(jnp.bfloat16)
    chunks = sems.shape[0]
    elements = fields.shape[1]
    per = elements // chunks
    copies = []
    for i in range(chunks):
        rows = slice(i * per * NODES, (i + 1) * per * NODES)
        here = slice(i * per, (i + 1) * per)
        total = own[rows, :] + jnp.dot(table[rows, :], arrived, preferred_element_type=jnp.float32)
        factor = np.float32(STEP_SIZE) / both_halves(total[:, MASS:])
        for f in range(3):
            moved = (total[:, f * LANES : (f + 1) * LANES] * factor).reshape(per, NODES, LANES)
            held[f, here] = (fields[f, here].astype(jnp.float32) + moved).astype(jnp.bfloat16)
        copy = pltpu.make_async_copy(
            held.at[:, pl.ds(i * per, per)], out.at[:, pl.ds(i * per, per)], sems.at[i]
        )
        copy.start()
        copies.append(copy)
    for copy in copies:
        copy.wait()


def in_hbm(value):
    return pltpu.with_memory_space_constraint(value, pltpu.HBM)


def call(kernel, outs, ins, args, scratch=(), limit=8 * MIB, flops=0):
    return pl.pallas_call(
        kernel,
        out_shape=[jax.ShapeDtypeStruct(shape, dtype) for shape, dtype, _ in outs],
        out_specs=[pl.BlockSpec(memory_space=space) for _, _, space in outs],
        in_specs=[pl.BlockSpec(memory_space=space) for space in ins],
        scratch_shapes=list(scratch),
        compiler_params=pltpu.CompilerParams(vmem_limit_bytes=limit),
        cost_estimate=pl.CostEstimate(flops=flops, bytes_accessed=0, transcendentals=0) if flops else None,
    )(*args)


def local(prognostic, metric, coriolis, node_point, send_point, recv_point):
    elements = prognostic.shape[1]
    levels = prognostic.shape[3]
    links = send_point.shape[0]
    plan = Plan(elements, links, 4 * lax.axis_size("sub"))
    rows = elements * NODES
    vm, hbm = pltpu.VMEM, pltpu.HBM
    f32, bf16 = jnp.float32, jnp.bfloat16
    send = send_point.reshape(1, links)
    recv = recv_point.reshape(1, links)
    metric = jnp.transpose(metric, (0, 2, 1))
    coriolis = jnp.transpose(coriolis)
    points = jnp.transpose(node_point)
    wide = 4 * levels
    sent = call(
        lambda *refs: tendency_kernel(plan, *refs),
        (
            (prognostic.shape, bf16, vm),
            ((rows, wide), bf16, vm),
            ((elements // SUB, LANES), f32, vm),
            (points.shape, jnp.int32, vm),
            (recv.shape, jnp.int32, vm),
        )
        + tuple(((plan.message_rows(group), LANES), f32, vm) for group in range(4)),
        (hbm,) * 6,
        tuple(in_hbm(x) for x in (prognostic, metric, coriolis, points, send, recv)),
        (
            vm(metric.shape, f32),
            vm(coriolis.shape, f32),
            vm(send.shape, jnp.int32),
            vm((elements // SUB, 3, SUB * NODES, levels), f32),
            vm((plan.rows, rows), bf16),
            vm((plan.rows, wide), f32),
            vm((5, rows, LANES), f32),
            pltpu.SemaphoreType.DMA((5,)),
            pltpu.SemaphoreType.DMA((4,)),
        ),
    )
    fields, weighted, numbers, points, recv = sent[:5]
    landed = []
    for group in range(4):
        landed.append(shift(sent[5 + group], plan.offsets[group]))
    own, table = call(
        lambda *refs: local_kernel(plan, *refs),
        (((rows, wide), f32, vm), ((rows, plan.width), bf16, vm)),
        (vm,) * 4,
        (weighted, numbers, points, recv),
    )
    relays = call(
        lambda *refs: relay_kernel(plan, *refs), (((SUB, LANES), f32, vm),) * 2, (vm, vm), (landed[0], landed[1])
    )
    passed = []
    for i, offset in enumerate((plan.lap, -plan.lap)):
        passed.append(shift(relays[i], offset))
    (advanced,) = call(
        lambda *refs: finish_kernel(plan, *refs),
        ((prognostic.shape, bf16, hbm),),
        (vm,) * 9,
        (fields, own, table, *landed, *passed),
        (
            vm(prognostic.shape, bf16),
            vm((plan.width, wide), f32),
            pltpu.SemaphoreType.DMA((4,)),
        ),
    )
    return advanced


def solution(mesh):
    placed = (
        P(None, AXES, None, None),
        P(None, AXES, None),
        P(AXES, None),
        P(AXES, None),
        P(AXES),
        P(AXES),
    )
    return jax.shard_map(
        local,
        mesh=mesh,
        in_specs=placed,
        out_specs=P(None, AXES, None, None),
        check_vma=False,
    )
```

```python
import math

import jax
import jax.numpy as jnp
import numpy as np
from jax import lax
from jax.experimental import pallas as pl
from jax.experimental.pallas import tpu as pltpu
from jax.sharding import PartitionSpec as P


STEP_SIZE = 0.1
AXES = ("face", "sub")
NODES = 16
SUB = 8
LANES = 128
MASS = 3 * LANES
MIB = 1024 * 1024
CARRIED = {0: (4, 7), 1: (6, 5)}
PASSED = ((4, 6), (7, 5))


def shift(value, steps):
    count = lax.axis_size(AXES)
    return lax.ppermute(value, AXES, [(d, (d + steps) % count) for d in range(count)])


def gll_tables():
    abscissa = np.array([-1.0, -math.sqrt(0.2), math.sqrt(0.2), 1.0])
    legendre = 0.5 * (5.0 * abscissa * abscissa * abscissa - 3.0 * abscissa)
    derivative = np.zeros((4, 4))
    for target in range(4):
        for source in range(4):
            if target != source:
                derivative[target, source] = legendre[target] / (
                    legendre[source] * (abscissa[target] - abscissa[source])
                )
    derivative[0, 0] = -3.0
    derivative[3, 3] = 3.0
    weights = np.array([1.0, 5.0, 5.0, 1.0]) / 6.0
    return (derivative, weights)


class Plan:
    def __init__(self, elements, links, lap):
        around = (links - 8) // 6
        short = 1
        while short * (around - short) < elements:
            short += 1
        side = 3 * short + 1
        top = 3 * (around - short) + 1
        first = [0]
        for count in (side, side, top, top, 1, 1, 1):
            first.append(first[-1] + count)
        self.offsets = (1, -1, lap, -lap, lap + 1, -lap - 1, lap - 1, 1 - lap)
        self.lap = lap
        self.tiles = top // SUB * SUB
        self.rest = top - self.tiles
        self.side_rows = -(-side // SUB) * SUB
        self.sides = 2 * self.tiles
        self.tail = self.sides + 2 * self.side_rows
        self.corner = self.tail + 2 * self.rest
        self.rows = -(-(self.corner + 4) // SUB) * SUB
        self.width = -(-self.rows // 256) * 256
        self.weight_rows = self.width // LANES
        self.spans = []
        for group in range(8):
            start = first[group]
            if group < 2:
                spans = ((start, self.sides + group * self.side_rows, side),)
            elif group < 4:
                spans = (
                    (start, (group - 2) * self.tiles, self.tiles),
                    (start + self.tiles, self.tail + (group - 2) * self.rest, self.rest),
                )
            else:
                spans = ((start, self.corner + group - 4, 1),)
            self.spans.append([span for span in spans if span[2]])

    def blocks(self, group):
        out = []
        place = 0
        for _, row, count in self.spans[group]:
            pitch = self.side_rows if group < 2 else count
            out.append((row, place, count, pitch))
            place += 3 * pitch
        for passed in CARRIED.get(group, ()):
            out.append((self.corner + passed - 4, place, 1, 1))
            place += 3
        return out

    def weight_row(self, group):
        _, place, _, pitch = self.blocks(group)[-1]
        return place + 3 * pitch

    def message_rows(self, group):
        return -(-(self.weight_row(group) + self.weight_rows) // SUB) * SUB

    def lanes(self, groups, index):
        at = iota((1, LANES), 1) + index * LANES
        mine = at < 0
        for group in groups:
            for _, row, count in self.spans[group]:
                mine = mine | ((at >= row) & (at < row + count))
        return mine


def iota(shape, axis):
    return lax.broadcasted_iota(jnp.int32, shape, axis)


def arranged(points_ref, plan):
    links = points_ref.shape[1]
    width = plan.width
    raw = points_ref[...].astype(jnp.float32)
    raw = jnp.concatenate([raw, jnp.full((1, width - links), -1.0, jnp.float32)], axis=1)
    raw = jnp.broadcast_to(raw, (SUB, width))
    lane = iota((SUB, width), 1)
    row = jnp.full((SUB, width), -1.0, jnp.float32)
    for spans in plan.spans:
        for source, target, count in spans:
            turned = pltpu.roll(raw, (target - source) % width, 1)
            row = jnp.where((lane >= target) & (lane < target + count), turned, row)
    return row[0:1]


def as_column(row, rows):
    width = row.shape[1]
    shape = (rows, width)
    return jnp.sum(jnp.where(iota(shape, 0) == iota(shape, 1), row, 0.0), axis=1, keepdims=True)


def as_row(column, width):
    shape = (column.shape[0], width)
    return jnp.sum(jnp.where(iota(shape, 0) == iota(shape, 1), column[:, :1], 0.0), axis=0, keepdims=True)


def point_rows(stack, first):
    elements = stack.shape[0]
    square = (LANES, LANES)
    spread = (iota(square, 1) // SUB + first == iota(square, 0)).astype(jnp.float32)
    wide = jnp.dot(stack, spread, precision=lax.Precision.HIGHEST, preferred_element_type=jnp.float32)
    mine = iota(wide.shape, 1) % SUB == iota(wide.shape, 0) % SUB
    return jnp.sum(jnp.where(mine, wide, 0.0).reshape(elements // SUB, SUB, LANES), axis=1)


def both_halves(mass):
    return mass + pltpu.roll(mass, LANES // 2, 1)


def split_lanes(mass):
    upper = mass.astype(jnp.bfloat16).astype(jnp.float32)
    return jnp.where(iota(mass.shape, 1) < LANES // 2, mass, mass - upper)


def derive(values, axis, scale, sign=1.0):
    table, _ = gll_tables()
    out = [None] * NODES
    for other in range(4):
        spot = (lambda i: 4 * other + i) if axis == 1 else (lambda i: 4 * i + other)
        x0, x1, x2, x3 = (values[spot(i)] for i in range(4))
        diff_a = x0 - x3
        diff_b = x1 - x2
        even = (x0 + x3) - (x1 + x2)
        for i in (0, 1):
            factor = sign * scale[other] * scale[i]
            p = even * np.float32(factor * 0.5 * (table[i, 0] + table[i, 3]))
            q = diff_a * np.float32(factor * 0.5 * (table[i, 0] - table[i, 3])) + diff_b * np.float32(
                factor * 0.5 * (table[i, 1] - table[i, 2])
            )
            out[spot(i)] = q + p
            out[spot(3 - i)] = q - p
    return out


def tendency_kernel(plan, *refs):
    prog, metric, cor, points, send, recv = refs[:6]
    fields, weighted, numbers, pts_v, recv_v = refs[6:11]
    messages = refs[11:15]
    met_v, cor_v, send_v, tile, mask, total, coefs, sems, chunk_sems = refs[15:]
    elements = fields.shape[1]
    groups = elements // SUB
    chunks = chunk_sems.shape[0]
    per = elements // chunks
    smalls = [
        pltpu.make_async_copy(source, target, sems.at[i])
        for i, (source, target) in enumerate(((points, pts_v), (send, send_v), (metric, met_v), (cor, cor_v)))
    ]
    for copy in smalls:
        copy.start()
    larges = [
        pltpu.make_async_copy(
            prog.at[:, pl.ds(i * per, per)], fields.at[:, pl.ds(i * per, per)], chunk_sems.at[i]
        )
        for i in range(chunks)
    ]
    for copy in larges:
        copy.start()
    later = pltpu.make_async_copy(recv, recv_v, sems.at[4])
    later.start()
    for copy in smalls:
        copy.wait()
    rows = plan.rows
    wanted = as_column(arranged(send_v, plan), rows)
    _, scale = gll_tables()
    a, b, e, g = (met_v[i] for i in range(4))
    node = iota(a.shape, 0)
    row_edge = (node // 4 == 0) | (node // 4 == 3)
    col_edge = (node % 4 == 0) | (node % 4 == 3)
    quad = jnp.where(row_edge, np.float32(scale[0]), np.float32(scale[1])) * jnp.where(
        col_edge, np.float32(scale[0]), np.float32(scale[1])
    )
    inv = 1.0 / (a * g - b * e)
    mass = quad * inv
    upper = mass.astype(jnp.bfloat16).astype(jnp.float32)
    stack = (a * inv, b * inv, e * inv, g * inv, mass * cor_v[...], upper, mass - upper, pts_v[...].astype(jnp.float32))
    stack = jnp.transpose(jnp.concatenate(stack, axis=0))
    numbers[...] = point_rows(stack, 7 * NODES)
    step = groups // chunks
    square = (LANES, LANES)
    kind = iota(square, 0) // NODES
    half = (iota(square, 1) >= LANES // 2).astype(jnp.int32)
    lift = [(kind == i).astype(jnp.bfloat16) for i in range(5)]
    fine = jnp.concatenate(lift + [jnp.zeros(square, jnp.bfloat16)], axis=1)
    lift = jnp.concatenate([jnp.concatenate(lift + [(kind == 5 + half).astype(jnp.bfloat16)], axis=1), fine], axis=0)
    coarse = stack.astype(jnp.bfloat16).astype(jnp.float32)
    slot = iota((SUB, LANES), 1) % NODES

    def lifted(i):
        for group in range(i * step, (i + 1) * step):
            here = slice(group * SUB, (group + 1) * SUB)
            picked = jnp.concatenate(
                [
                    jnp.concatenate([jnp.where(slot == k, part[here], 0.0) for k in range(NODES)], axis=0)
                    for part in (coarse, stack - coarse)
                ],
                axis=1,
            ).astype(jnp.bfloat16)
            there = slice(group * LANES, (group + 1) * LANES)
            wide = jnp.dot(picked, lift, preferred_element_type=jnp.float32)
            for which in range(5):
                coefs[which, there, :] = wide[:, which * LANES : (which + 1) * LANES]
            weighted[there, MASS:] = wide[:, 5 * LANES :].astype(jnp.bfloat16)

    lifted(0)
    for group in range(groups):
        mask[:, group * LANES : (group + 1) * LANES] = (
            jnp.broadcast_to(wanted, (rows, LANES)) == numbers[group : group + 1, :]
        ).astype(jnp.bfloat16)

    def body(group):
        ca, cb, ce, cg, cf = (
            [coefs[i, (group * NODES + k) * SUB : (group * NODES + k + 1) * SUB, :] for k in range(NODES)]
            for i in range(5)
        )
        u, v, h = ([tile[group, f, k * SUB : (k + 1) * SUB, :] for k in range(NODES)] for f in range(3))
        span = range(NODES)
        energy = [0.5 * (u[k] * u[k] + v[k] * v[k]) + h[k] for k in span]
        along = derive(energy, 1, scale, -1.0)
        across = derive(energy, 0, scale, -1.0)
        grad_one = [ca[k] * along[k] + ce[k] * across[k] for k in span]
        grad_two = [cb[k] * along[k] + cg[k] * across[k] for k in span]
        turn_two = derive([ca[k] * v[k] - cb[k] * u[k] for k in span], 1, scale)
        turn_one = derive([cg[k] * u[k] - ce[k] * v[k] for k in span], 0, scale)
        eta = [turn_two[k] - turn_one[k] + cf[k] for k in span]
        flow_one = derive([h[k] * (ca[k] * u[k] + cb[k] * v[k]) for k in span], 1, scale, -1.0)
        flow_two = derive([h[k] * (ce[k] * u[k] + cg[k] * v[k]) for k in span], 0, scale, -1.0)
        parts = (
            [eta[k] * v[k] + grad_one[k] for k in span],
            [grad_two[k] - eta[k] * u[k] for k in span],
            [flow_one[k] + flow_two[k] for k in span],
        )
        there = slice(group * LANES, (group + 1) * LANES)
        for f, part in enumerate(parts):
            weighted[there, f * LANES : (f + 1) * LANES] = jnp.concatenate(part, axis=0).astype(jnp.bfloat16)

    turn = (
        iota(square, 1) == iota(square, 0) % SUB * NODES + iota(square, 0) // SUB
    ).astype(jnp.bfloat16)

    def reorder(i):
        for group in range(i * step, (i + 1) * step):
            here = slice(group * SUB, (group + 1) * SUB)
            for f in range(3):
                tile[group, f] = jnp.dot(
                    turn, fields[f, here].reshape(SUB * NODES, LANES), preferred_element_type=jnp.float32
                )

    def gather(i):
        span = slice(i * step * LANES, (i + 1) * step * LANES)
        part = jnp.dot(mask[:, span], weighted[span, :], preferred_element_type=jnp.float32)
        total[...] = part if i == 0 else total[...] + part

    for copy in larges:
        copy.wait()
    reorder(0)
    for i in range(chunks):
        for group in range(i * step, (i + 1) * step):
            body(group)
        if i:
            gather(i - 1)
        if i + 1 < chunks:
            reorder(i + 1)
            lifted(i + 1)
    gather(chunks - 1)
    later.wait()
    sums = total[...]
    masses = as_row(both_halves(sums[:, MASS:]), plan.width)
    for group, ref in enumerate(messages):
        ref[ref.shape[0] - SUB :, :] = jnp.zeros((SUB, LANES), jnp.float32)
        for row, place, count, pitch in plan.blocks(group):
            span = pitch if pitch > count else count
            for f in range(3):
                ref[place + f * pitch : place + f * pitch + span, :] = sums[
                    row : row + span, f * LANES : (f + 1) * LANES
                ]
        for index in range(plan.weight_rows):
            mine = plan.lanes((group, *CARRIED.get(group, ())), index)
            at = plan.weight_row(group) + index
            ref[at : at + 1, :] = jnp.where(mine, masses[:, index * LANES : (index + 1) * LANES], 0.0)


def point_columns(points, group):
    return jnp.concatenate(
        [
            jnp.broadcast_to(points[:, e : e + 1], (NODES, LANES))
            for e in range(group * SUB, (group + 1) * SUB)
        ],
        axis=0,
    )


def local_sums(points, numbers, weighted, own):
    groups = weighted.shape[0] // LANES
    tall = SUB * NODES
    for i in range(own.shape[0] // tall):
        column = point_columns(points, i)
        same = jnp.concatenate(
            [(column == numbers[j : j + 1, :]).astype(jnp.bfloat16) for j in range(groups)], axis=1
        )
        own[i * tall : (i + 1) * tall, :] = jnp.dot(same, weighted[...], preferred_element_type=jnp.float32)


def local_kernel(plan, weighted, numbers, points, recv, own, table):
    landing = arranged(recv, plan)
    values = points[...].astype(jnp.float32)
    tall = SUB * NODES
    for group in range(numbers.shape[0]):
        column = point_columns(values, group)
        for i in range(0, plan.width, LANES):
            table[group * tall : (group + 1) * tall, i : i + LANES] = (
                column == landing[:, i : i + LANES]
            ).astype(jnp.bfloat16)
    local_sums(values, numbers, weighted, own)


def relay_kernel(plan, left, right, up, down):
    start = plan.weight_row(0)
    for i, ref in enumerate((up, down)):
        place = plan.blocks(0)[-2 + i][1]
        ref[0:3, :] = left[place : place + 3, :]
        ref[3:6, :] = right[place : place + 3, :]
        for index in range(plan.weight_rows):
            at = slice(start + index, start + index + 1)
            ref[6 + index : 7 + index, :] = jnp.where(
                plan.lanes(PASSED[i][:1], index), left[at, :], 0.0
            ) + jnp.where(plan.lanes(PASSED[i][1:], index), right[at, :], 0.0)


def finish_kernel(plan, fields, own, table, *refs):
    messages = refs[:4]
    relays = refs[4:6]
    out, held, landed, sems = refs[6:]
    width = plan.width
    landed[plan.tail :, :] = jnp.zeros((width - plan.tail, landed.shape[1]), jnp.float32)
    weights = []
    for index in range(plan.weight_rows):
        parts = [ref[6 + index : 7 + index, :] for ref in relays]
        for group, ref in enumerate(messages):
            at = plan.weight_row(group) + index
            row = ref[at : at + 1, :]
            parts.append(jnp.where(plan.lanes((group,), index), row, 0.0) if group < 2 else row)
        weights.append(sum(parts[1:], parts[0]))
    masses = as_column(jnp.concatenate(weights, axis=1), width)
    for group, ref in enumerate(messages):
        for row, place, count, pitch in plan.blocks(group)[: len(plan.spans[group])]:
            span = pitch if pitch > count else count
            for f in range(3):
                landed[row : row + span, f * LANES : (f + 1) * LANES] = ref[
                    place + f * pitch : place + f * pitch + span, :
                ]
    for passed, ref in zip(PASSED, relays):
        for i, group in enumerate(passed):
            row = plan.corner + group - 4
            for f in range(3):
                landed[row : row + 1, f * LANES : (f + 1) * LANES] = ref[3 * i + f : 3 * i + f + 1, :]
    landed[:, MASS:] = split_lanes(jnp.broadcast_to(masses, (width, LANES)))
    arrived = landed[...].astype(jnp.bfloat16)
    chunks = sems.shape[0]
    elements = fields.shape[1]
    per = elements // chunks
    copies = []
    for i in range(chunks):
        rows = slice(i * per * NODES, (i + 1) * per * NODES)
        here = slice(i * per, (i + 1) * per)
        total = own[rows, :] + jnp.dot(table[rows, :], arrived, preferred_element_type=jnp.float32)
        factor = np.float32(STEP_SIZE) / both_halves(total[:, MASS:])
        for f in range(3):
            moved = (total[:, f * LANES : (f + 1) * LANES] * factor).reshape(per, NODES, LANES)
            held[f, here] = (fields[f, here].astype(jnp.float32) + moved).astype(jnp.bfloat16)
        copy = pltpu.make_async_copy(
            held.at[:, pl.ds(i * per, per)], out.at[:, pl.ds(i * per, per)], sems.at[i]
        )
        copy.start()
        copies.append(copy)
    for copy in copies:
        copy.wait()


def in_hbm(value):
    return pltpu.with_memory_space_constraint(value, pltpu.HBM)


def call(kernel, outs, ins, args, scratch=(), limit=8 * MIB, flops=0):
    return pl.pallas_call(
        kernel,
        out_shape=[jax.ShapeDtypeStruct(shape, dtype) for shape, dtype, _ in outs],
        out_specs=[pl.BlockSpec(memory_space=space) for _, _, space in outs],
        in_specs=[pl.BlockSpec(memory_space=space) for space in ins],
        scratch_shapes=list(scratch),
        compiler_params=pltpu.CompilerParams(vmem_limit_bytes=limit),
        cost_estimate=pl.CostEstimate(flops=flops, bytes_accessed=0, transcendentals=0) if flops else None,
    )(*args)


def local(prognostic, metric, coriolis, node_point, send_point, recv_point):
    elements = prognostic.shape[1]
    levels = prognostic.shape[3]
    links = send_point.shape[0]
    plan = Plan(elements, links, 4 * lax.axis_size("sub"))
    rows = elements * NODES
    vm, hbm = pltpu.VMEM, pltpu.HBM
    f32, bf16 = jnp.float32, jnp.bfloat16
    send = send_point.reshape(1, links)
    recv = recv_point.reshape(1, links)
    metric = jnp.transpose(metric, (0, 2, 1))
    coriolis = jnp.transpose(coriolis)
    points = jnp.transpose(node_point)
    wide = 4 * levels
    sent = call(
        lambda *refs: tendency_kernel(plan, *refs),
        (
            (prognostic.shape, bf16, vm),
            ((rows, wide), bf16, vm),
            ((elements // SUB, LANES), f32, vm),
            (points.shape, jnp.int32, vm),
            (recv.shape, jnp.int32, vm),
        )
        + tuple(((plan.message_rows(group), LANES), f32, vm) for group in range(4)),
        (hbm,) * 6,
        tuple(in_hbm(x) for x in (prognostic, metric, coriolis, points, send, recv)),
        (
            vm(metric.shape, f32),
            vm(coriolis.shape, f32),
            vm(send.shape, jnp.int32),
            vm((elements // SUB, 3, SUB * NODES, levels), f32),
            vm((plan.rows, rows), bf16),
            vm((plan.rows, wide), f32),
            vm((5, rows, LANES), f32),
            pltpu.SemaphoreType.DMA((5,)),
            pltpu.SemaphoreType.DMA((4,)),
        ),
    )
    fields, weighted, numbers, points, recv = sent[:5]
    landed = []
    for group in range(4):
        landed.append(shift(sent[5 + group], plan.offsets[group]))
    own, table = call(
        lambda *refs: local_kernel(plan, *refs),
        (((rows, wide), f32, vm), ((rows, plan.width), bf16, vm)),
        (vm,) * 4,
        (weighted, numbers, points, recv),
    )
    relays = call(
        lambda *refs: relay_kernel(plan, *refs), (((SUB, LANES), f32, vm),) * 2, (vm, vm), (landed[0], landed[1])
    )
    passed = []
    for i, offset in enumerate((plan.lap, -plan.lap)):
        passed.append(shift(relays[i], offset))
    (advanced,) = call(
        lambda *refs: finish_kernel(plan, *refs),
        ((prognostic.shape, bf16, hbm),),
        (vm,) * 9,
        (fields, own, table, *landed, *passed),
        (
            vm(prognostic.shape, bf16),
            vm((plan.width, wide), f32),
            pltpu.SemaphoreType.DMA((4,)),
        ),
    )
    return advanced


def solution(mesh):
    placed = (
        P(None, AXES, None, None),
        P(None, AXES, None),
        P(AXES, None),
        P(AXES, None),
        P(AXES),
        P(AXES),
    )
    return jax.shard_map(
        local,
        mesh=mesh,
        in_specs=placed,
        out_specs=P(None, AXES, None, None),
        check_vma=False,
    )
```

```python
import math

import jax
import jax.numpy as jnp
import numpy as np
from jax import lax
from jax.experimental import pallas as pl
from jax.experimental.pallas import tpu as pltpu
from jax.sharding import PartitionSpec as P


STEP_SIZE = 0.1
AXES = ("face", "sub")
NODES = 16
SUB = 8
LANES = 128
MASS = 3 * LANES
MIB = 1024 * 1024
CARRIED = {0: (4, 7), 1: (6, 5)}
PASSED = ((4, 6), (7, 5))


def shift(value, steps):
    count = lax.axis_size(AXES)
    return lax.ppermute(value, AXES, [(d, (d + steps) % count) for d in range(count)])


def gll_tables():
    abscissa = np.array([-1.0, -math.sqrt(0.2), math.sqrt(0.2), 1.0])
    legendre = 0.5 * (5.0 * abscissa * abscissa * abscissa - 3.0 * abscissa)
    derivative = np.zeros((4, 4))
    for target in range(4):
        for source in range(4):
            if target != source:
                derivative[target, source] = legendre[target] / (
                    legendre[source] * (abscissa[target] - abscissa[source])
                )
    derivative[0, 0] = -3.0
    derivative[3, 3] = 3.0
    weights = np.array([1.0, 5.0, 5.0, 1.0]) / 6.0
    return (derivative, weights)


class Plan:
    def __init__(self, elements, links, lap):
        around = (links - 8) // 6
        short = 1
        while short * (around - short) < elements:
            short += 1
        side = 3 * short + 1
        top = 3 * (around - short) + 1
        first = [0]
        for count in (side, side, top, top, 1, 1, 1):
            first.append(first[-1] + count)
        self.offsets = (1, -1, lap, -lap, lap + 1, -lap - 1, lap - 1, 1 - lap)
        self.lap = lap
        self.tiles = top // SUB * SUB
        self.rest = top - self.tiles
        self.side_rows = -(-side // SUB) * SUB
        self.sides = 2 * self.tiles
        self.tail = self.sides + 2 * self.side_rows
        self.corner = self.tail + 2 * self.rest
        self.rows = -(-(self.corner + 4) // SUB) * SUB
        self.width = -(-self.rows // 256) * 256
        self.weight_rows = self.width // LANES
        self.spans = []
        for group in range(8):
            start = first[group]
            if group < 2:
                spans = ((start, self.sides + group * self.side_rows, side),)
            elif group < 4:
                spans = (
                    (start, (group - 2) * self.tiles, self.tiles),
                    (start + self.tiles, self.tail + (group - 2) * self.rest, self.rest),
                )
            else:
                spans = ((start, self.corner + group - 4, 1),)
            self.spans.append([span for span in spans if span[2]])

    def blocks(self, group):
        out = []
        place = 0
        for _, row, count in self.spans[group]:
            pitch = self.side_rows if group < 2 else count
            out.append((row, place, count, pitch))
            place += 3 * pitch
        for passed in CARRIED.get(group, ()):
            out.append((self.corner + passed - 4, place, 1, 1))
            place += 3
        return out

    def weight_row(self, group):
        _, place, _, pitch = self.blocks(group)[-1]
        return place + 3 * pitch

    def message_rows(self, group):
        return -(-(self.weight_row(group) + self.weight_rows) // SUB) * SUB

    def lanes(self, groups, index):
        at = iota((1, LANES), 1) + index * LANES
        mine = at < 0
        for group in groups:
            for _, row, count in self.spans[group]:
                mine = mine | ((at >= row) & (at < row + count))
        return mine


def iota(shape, axis):
    return lax.broadcasted_iota(jnp.int32, shape, axis)


def arranged(points_ref, plan):
    links = points_ref.shape[1]
    width = plan.width
    raw = points_ref[...].astype(jnp.float32)
    raw = jnp.concatenate([raw, jnp.full((1, width - links), -1.0, jnp.float32)], axis=1)
    raw = jnp.broadcast_to(raw, (SUB, width))
    lane = iota((SUB, width), 1)
    row = jnp.full((SUB, width), -1.0, jnp.float32)
    for spans in plan.spans:
        for source, target, count in spans:
            turned = pltpu.roll(raw, (target - source) % width, 1)
            row = jnp.where((lane >= target) & (lane < target + count), turned, row)
    return row[0:1]


def as_column(row, rows):
    width = row.shape[1]
    shape = (rows, width)
    return jnp.sum(jnp.where(iota(shape, 0) == iota(shape, 1), row, 0.0), axis=1, keepdims=True)


def as_row(column, width):
    shape = (column.shape[0], width)
    return jnp.sum(jnp.where(iota(shape, 0) == iota(shape, 1), column[:, :1], 0.0), axis=0, keepdims=True)


def point_rows(stack, first):
    elements = stack.shape[0]
    square = (LANES, LANES)
    spread = (iota(square, 1) // SUB + first == iota(square, 0)).astype(jnp.float32)
    wide = jnp.dot(stack, spread, precision=lax.Precision.HIGHEST, preferred_element_type=jnp.float32)
    mine = iota(wide.shape, 1) % SUB == iota(wide.shape, 0) % SUB
    return jnp.sum(jnp.where(mine, wide, 0.0).reshape(elements // SUB, SUB, LANES), axis=1)


def both_halves(mass):
    return mass + pltpu.roll(mass, LANES // 2, 1)


def split_lanes(mass):
    upper = mass.astype(jnp.bfloat16).astype(jnp.float32)
    return jnp.where(iota(mass.shape, 1) < LANES // 2, mass, mass - upper)


def derive(values, axis, scale, sign=1.0):
    table, _ = gll_tables()
    out = [None] * NODES
    for other in range(4):
        spot = (lambda i: 4 * other + i) if axis == 1 else (lambda i: 4 * i + other)
        x0, x1, x2, x3 = (values[spot(i)] for i in range(4))
        diff_a = x0 - x3
        diff_b = x1 - x2
        even = (x0 + x3) - (x1 + x2)
        for i in (0, 1):
            factor = sign * scale[other] * scale[i]
            p = even * np.float32(factor * 0.5 * (table[i, 0] + table[i, 3]))
            q = diff_a * np.float32(factor * 0.5 * (table[i, 0] - table[i, 3])) + diff_b * np.float32(
                factor * 0.5 * (table[i, 1] - table[i, 2])
            )
            out[spot(i)] = q + p
            out[spot(3 - i)] = q - p
    return out


def tendency_kernel(plan, *refs):
    prog, metric, cor, points, send, recv = refs[:6]
    fields, weighted, numbers, pts_v, recv_v = refs[6:11]
    messages = refs[11:15]
    met_v, cor_v, send_v, tile, mask, total, coefs, sems, chunk_sems = refs[15:]
    elements = fields.shape[1]
    groups = elements // SUB
    chunks = 4
    cuts = chunk_sems.shape[0]
    per = elements // cuts
    smalls = [
        pltpu.make_async_copy(source, target, sems.at[i])
        for i, (source, target) in enumerate(((points, pts_v), (send, send_v), (metric, met_v), (cor, cor_v)))
    ]
    for copy in smalls:
        copy.start()
    larges = [
        pltpu.make_async_copy(
            prog.at[:, pl.ds(i * per, per)], fields.at[:, pl.ds(i * per, per)], chunk_sems.at[i]
        )
        for i in range(cuts)
    ]
    for copy in larges:
        copy.start()
    later = pltpu.make_async_copy(recv, recv_v, sems.at[4])
    later.start()
    for copy in smalls:
        copy.wait()
    rows = plan.rows
    wanted = as_column(arranged(send_v, plan), rows)
    _, scale = gll_tables()
    a, b, e, g = (met_v[i] for i in range(4))
    node = iota(a.shape, 0)
    row_edge = (node // 4 == 0) | (node // 4 == 3)
    col_edge = (node % 4 == 0) | (node % 4 == 3)
    quad = jnp.where(row_edge, np.float32(scale[0]), np.float32(scale[1])) * jnp.where(
        col_edge, np.float32(scale[0]), np.float32(scale[1])
    )
    inv = 1.0 / (a * g - b * e)
    mass = quad * inv
    share = mass * np.float32(1.0 / STEP_SIZE)
    upper = share.astype(jnp.bfloat16).astype(jnp.float32)
    stack = (a * inv, b * inv, e * inv, g * inv, mass * cor_v[...], upper, share - upper, pts_v[...].astype(jnp.float32))
    stack = jnp.transpose(jnp.concatenate(stack, axis=0))
    numbers[...] = point_rows(stack, 7 * NODES)
    step = groups // chunks
    square = (LANES, LANES)
    kind = iota(square, 0) // NODES
    half = (iota(square, 1) >= LANES // 2).astype(jnp.int32)
    lift = [(kind == i).astype(jnp.bfloat16) for i in range(5)]
    fine = jnp.concatenate(lift + [jnp.zeros(square, jnp.bfloat16)], axis=1)
    lift = jnp.concatenate([jnp.concatenate(lift + [(kind == 5 + half).astype(jnp.bfloat16)], axis=1), fine], axis=0)
    coarse = stack.astype(jnp.bfloat16).astype(jnp.float32)
    slot = iota((SUB, LANES), 1) % NODES

    def lifted(i):
        for group in range(i * step, (i + 1) * step):
            here = slice(group * SUB, (group + 1) * SUB)
            picked = jnp.concatenate(
                [
                    jnp.concatenate([jnp.where(slot == k, part[here], 0.0) for k in range(NODES)], axis=0)
                    for part in (coarse, stack - coarse)
                ],
                axis=1,
            ).astype(jnp.bfloat16)
            there = slice(group * LANES, (group + 1) * LANES)
            wide = jnp.dot(picked, lift, preferred_element_type=jnp.float32)
            for which in range(5):
                coefs[which, there, :] = wide[:, which * LANES : (which + 1) * LANES]
            weighted[there, MASS:] = wide[:, 5 * LANES :].astype(jnp.bfloat16)

    lifted(0)
    for group in range(groups):
        mask[:, group * LANES : (group + 1) * LANES] = (
            jnp.broadcast_to(wanted, (rows, LANES)) == numbers[group : group + 1, :]
        ).astype(jnp.bfloat16)

    def body(group):
        ca, cb, ce, cg, cf = (
            [coefs[i, (group * NODES + k) * SUB : (group * NODES + k + 1) * SUB, :] for k in range(NODES)]
            for i in range(5)
        )
        u, v, h = ([tile[group, f, k * SUB : (k + 1) * SUB, :] for k in range(NODES)] for f in range(3))
        span = range(NODES)
        energy = [u[k] * u[k] + v[k] * v[k] + h[k] for k in span]
        along = derive(energy, 1, scale, -0.5)
        across = derive(energy, 0, scale, -0.5)
        grad_one = [ca[k] * along[k] + ce[k] * across[k] for k in span]
        grad_two = [cb[k] * along[k] + cg[k] * across[k] for k in span]
        turn_two = derive([ca[k] * v[k] - cb[k] * u[k] for k in span], 1, scale)
        turn_one = derive([cg[k] * u[k] - ce[k] * v[k] for k in span], 0, scale)
        eta = [turn_two[k] - turn_one[k] + cf[k] for k in span]
        flow_one = derive([h[k] * (ca[k] * u[k] + cb[k] * v[k]) for k in span], 1, scale, -0.5)
        flow_two = derive([h[k] * (ce[k] * u[k] + cg[k] * v[k]) for k in span], 0, scale, -0.5)
        parts = (
            [eta[k] * v[k] + grad_one[k] for k in span],
            [grad_two[k] - eta[k] * u[k] for k in span],
            [flow_one[k] + flow_two[k] for k in span],
        )
        there = slice(group * LANES, (group + 1) * LANES)
        for f, part in enumerate(parts):
            weighted[there, f * LANES : (f + 1) * LANES] = jnp.concatenate(part, axis=0).astype(jnp.bfloat16)

    turn = (
        iota(square, 1) == iota(square, 0) % SUB * NODES + iota(square, 0) // SUB
    ).astype(jnp.bfloat16)

    def reorder(i):
        for group in range(i * step, (i + 1) * step):
            here = slice(group * SUB, (group + 1) * SUB)
            for f in range(3):
                tile[group, f] = jnp.dot(
                    turn if f < 2 else 2.0 * turn, fields[f, here].reshape(SUB * NODES, LANES), preferred_element_type=jnp.float32
                )

    def gather(i):
        span = slice(i * step * LANES, (i + 1) * step * LANES)
        part = jnp.dot(mask[:, span], weighted[span, :], preferred_element_type=jnp.float32)
        return part if i == 0 else total[...] + part

    for copy in larges:
        copy.wait()
    reorder(0)
    for i in range(chunks):
        for group in range(i * step, (i + 1) * step):
            body(group)
        if i:
            total[...] = gather(i - 1)
        if i + 1 < chunks:
            reorder(i + 1)
            lifted(i + 1)
    later.wait()
    sums = gather(chunks - 1)
    masses = as_row(both_halves(sums[:, MASS:]), plan.width)
    for group, ref in enumerate(messages):
        ref[ref.shape[0] - SUB :, :] = jnp.zeros((SUB, LANES), jnp.float32)
        for row, place, count, pitch in plan.blocks(group):
            span = pitch if pitch > count else count
            for f in range(3):
                ref[place + f * pitch : place + f * pitch + span, :] = sums[
                    row : row + span, f * LANES : (f + 1) * LANES
                ]
        for index in range(plan.weight_rows):
            mine = plan.lanes((group, *CARRIED.get(group, ())), index)
            at = plan.weight_row(group) + index
            ref[at : at + 1, :] = jnp.where(mine, masses[:, index * LANES : (index + 1) * LANES], 0.0)


def point_columns(points, group):
    return jnp.concatenate(
        [
            jnp.broadcast_to(points[:, e : e + 1], (NODES, LANES))
            for e in range(group * SUB, (group + 1) * SUB)
        ],
        axis=0,
    )


def local_sums(points, numbers, weighted, own):
    groups = weighted.shape[0] // LANES
    tall = SUB * NODES
    for i in range(own.shape[0] // tall):
        column = point_columns(points, i)
        same = jnp.concatenate(
            [(column == numbers[j : j + 1, :]).astype(jnp.bfloat16) for j in range(groups)], axis=1
        )
        own[i * tall : (i + 1) * tall, :] = jnp.dot(same, weighted[...], preferred_element_type=jnp.float32)


def local_kernel(plan, weighted, numbers, points, recv, own, table):
    landing = arranged(recv, plan)
    values = points[...].astype(jnp.float32)
    tall = SUB * NODES
    for group in range(numbers.shape[0]):
        column = point_columns(values, group)
        for i in range(0, plan.width, LANES):
            table[group * tall : (group + 1) * tall, i : i + LANES] = (
                column == landing[:, i : i + LANES]
            ).astype(jnp.bfloat16)
    local_sums(values, numbers, weighted, own)


def relay_kernel(plan, left, right, up, down):
    start = plan.weight_row(0)
    for i, ref in enumerate((up, down)):
        place = plan.blocks(0)[-2 + i][1]
        ref[0:3, :] = left[place : place + 3, :]
        ref[3:6, :] = right[place : place + 3, :]
        for index in range(plan.weight_rows):
            at = slice(start + index, start + index + 1)
            ref[6 + index : 7 + index, :] = jnp.where(
                plan.lanes(PASSED[i][:1], index), left[at, :], 0.0
            ) + jnp.where(plan.lanes(PASSED[i][1:], index), right[at, :], 0.0)


def finish_kernel(plan, fields, own, table, *refs):
    messages = refs[:4]
    relays = refs[4:6]
    out, held, landed, sems = refs[6:]
    width = plan.width
    landed[plan.tail :, :] = jnp.zeros((width - plan.tail, landed.shape[1]), jnp.float32)
    weights = []
    for index in range(plan.weight_rows):
        parts = [ref[6 + index : 7 + index, :] for ref in relays]
        for group, ref in enumerate(messages):
            at = plan.weight_row(group) + index
            row = ref[at : at + 1, :]
            parts.append(jnp.where(plan.lanes((group,), index), row, 0.0) if group < 2 else row)
        weights.append(sum(parts[1:], parts[0]))
    masses = as_column(jnp.concatenate(weights, axis=1), width)
    for group, ref in enumerate(messages):
        for row, place, count, pitch in plan.blocks(group)[: len(plan.spans[group])]:
            span = pitch if pitch > count else count
            for f in range(3):
                landed[row : row + span, f * LANES : (f + 1) * LANES] = ref[
                    place + f * pitch : place + f * pitch + span, :
                ]
    for passed, ref in zip(PASSED, relays):
        for i, group in enumerate(passed):
            row = plan.corner + group - 4
            for f in range(3):
                landed[row : row + 1, f * LANES : (f + 1) * LANES] = ref[3 * i + f : 3 * i + f + 1, :]
    landed[:, MASS:] = split_lanes(jnp.broadcast_to(masses, (width, LANES)))
    arrived = landed[...].astype(jnp.bfloat16)
    chunks = sems.shape[0]
    elements = fields.shape[1]
    per = elements // chunks
    copies = []
    for i in range(chunks):
        rows = slice(i * per * NODES, (i + 1) * per * NODES)
        here = slice(i * per, (i + 1) * per)
        total = own[rows, :] + jnp.dot(table[rows, :], arrived, preferred_element_type=jnp.float32)
        factor = 1.0 / both_halves(total[:, MASS:])
        for f in range(3):
            moved = (total[:, f * LANES : (f + 1) * LANES] * factor).reshape(per, NODES, LANES)
            held[f, here] = (fields[f, here].astype(jnp.float32) + moved).astype(jnp.bfloat16)
        copy = pltpu.make_async_copy(
            held.at[:, pl.ds(i * per, per)], out.at[:, pl.ds(i * per, per)], sems.at[i]
        )
        copy.start()
        copies.append(copy)
    for copy in copies:
        copy.wait()


def in_hbm(value):
    return pltpu.with_memory_space_constraint(value, pltpu.HBM)


def call(kernel, outs, ins, args, scratch=(), limit=8 * MIB, flops=0):
    return pl.pallas_call(
        kernel,
        out_shape=[jax.ShapeDtypeStruct(shape, dtype) for shape, dtype, _ in outs],
        out_specs=[pl.BlockSpec(memory_space=space) for _, _, space in outs],
        in_specs=[pl.BlockSpec(memory_space=space) for space in ins],
        scratch_shapes=list(scratch),
        compiler_params=pltpu.CompilerParams(vmem_limit_bytes=limit),
        cost_estimate=pl.CostEstimate(flops=flops, bytes_accessed=0, transcendentals=0) if flops else None,
    )(*args)


def local(prognostic, metric, coriolis, node_point, send_point, recv_point):
    elements = prognostic.shape[1]
    levels = prognostic.shape[3]
    links = send_point.shape[0]
    plan = Plan(elements, links, 4 * lax.axis_size("sub"))
    rows = elements * NODES
    vm, hbm = pltpu.VMEM, pltpu.HBM
    f32, bf16 = jnp.float32, jnp.bfloat16
    send = send_point.reshape(1, links)
    recv = recv_point.reshape(1, links)
    metric = jnp.transpose(metric, (0, 2, 1))
    coriolis = jnp.transpose(coriolis)
    points = jnp.transpose(node_point)
    wide = 4 * levels
    sent = call(
        lambda *refs: tendency_kernel(plan, *refs),
        (
            (prognostic.shape, bf16, vm),
            ((rows, wide), bf16, vm),
            ((elements // SUB, LANES), f32, vm),
            (points.shape, jnp.int32, vm),
            (recv.shape, jnp.int32, vm),
        )
        + tuple(((plan.message_rows(group), LANES), f32, vm) for group in range(4)),
        (hbm,) * 6,
        tuple(in_hbm(x) for x in (prognostic, metric, coriolis, points, send, recv)),
        (
            vm(metric.shape, f32),
            vm(coriolis.shape, f32),
            vm(send.shape, jnp.int32),
            vm((elements // SUB, 3, SUB * NODES, levels), f32),
            vm((plan.rows, rows), bf16),
            vm((plan.rows, wide), f32),
            vm((5, rows, LANES), f32),
            pltpu.SemaphoreType.DMA((5,)),
            pltpu.SemaphoreType.DMA((1,)),
        ),
    )
    fields, weighted, numbers, points, recv = sent[:5]
    landed = []
    for group in range(4):
        landed.append(shift(sent[5 + group], plan.offsets[group]))
    own, table = call(
        lambda *refs: local_kernel(plan, *refs),
        (((rows, wide), f32, vm), ((rows, plan.width), bf16, vm)),
        (vm,) * 4,
        (weighted, numbers, points, recv),
    )
    relays = call(
        lambda *refs: relay_kernel(plan, *refs), (((SUB, LANES), f32, vm),) * 2, (vm, vm), (landed[0], landed[1])
    )
    passed = []
    for i, offset in enumerate((plan.lap, -plan.lap)):
        passed.append(shift(relays[i], offset))
    (advanced,) = call(
        lambda *refs: finish_kernel(plan, *refs),
        ((prognostic.shape, bf16, hbm),),
        (vm,) * 9,
        (fields, own, table, *landed, *passed),
        (
            vm(prognostic.shape, bf16),
            vm((plan.width, wide), f32),
            pltpu.SemaphoreType.DMA((4,)),
        ),
    )
    return advanced


def solution(mesh):
    placed = (
        P(None, AXES, None, None),
        P(None, AXES, None),
        P(AXES, None),
        P(AXES, None),
        P(AXES),
        P(AXES),
    )
    return jax.shard_map(
        local,
        mesh=mesh,
        in_specs=placed,
        out_specs=P(None, AXES, None, None),
        check_vma=False,
    )
```

```python
import math

import jax
import jax.numpy as jnp
import numpy as np
from jax import lax
from jax.experimental import pallas as pl
from jax.experimental.pallas import tpu as pltpu
from jax.sharding import PartitionSpec as P


STEP_SIZE = 0.1
AXES = ("face", "sub")
NODES = 16
SUB = 8
LANES = 128
MASS = 3 * LANES
MIB = 1024 * 1024
CARRIED = {0: (4, 7), 1: (6, 5)}
PASSED = ((4, 6), (7, 5))


def shift(value, steps):
    count = lax.axis_size(AXES)
    return lax.ppermute(value, AXES, [(d, (d + steps) % count) for d in range(count)])


def gll_tables():
    abscissa = np.array([-1.0, -math.sqrt(0.2), math.sqrt(0.2), 1.0])
    legendre = 0.5 * (5.0 * abscissa * abscissa * abscissa - 3.0 * abscissa)
    derivative = np.zeros((4, 4))
    for target in range(4):
        for source in range(4):
            if target != source:
                derivative[target, source] = legendre[target] / (
                    legendre[source] * (abscissa[target] - abscissa[source])
                )
    derivative[0, 0] = -3.0
    derivative[3, 3] = 3.0
    weights = np.array([1.0, 5.0, 5.0, 1.0]) / 6.0
    return (derivative, weights)


class Plan:
    def __init__(self, elements, links, lap):
        around = (links - 8) // 6
        short = 1
        while short * (around - short) < elements:
            short += 1
        side = 3 * short + 1
        top = 3 * (around - short) + 1
        first = [0]
        for count in (side, side, top, top, 1, 1, 1):
            first.append(first[-1] + count)
        self.offsets = (1, -1, lap, -lap, lap + 1, -lap - 1, lap - 1, 1 - lap)
        self.lap = lap
        self.tiles = top // SUB * SUB
        self.rest = top - self.tiles
        self.side_rows = -(-side // SUB) * SUB
        self.sides = 2 * self.tiles
        self.tail = self.sides + 2 * self.side_rows
        self.corner = self.tail + 2 * self.rest
        self.rows = -(-(self.corner + 4) // SUB) * SUB
        self.width = -(-self.rows // 256) * 256
        self.weight_rows = self.width // LANES
        self.spans = []
        for group in range(8):
            start = first[group]
            if group < 2:
                spans = ((start, self.sides + group * self.side_rows, side),)
            elif group < 4:
                spans = (
                    (start, (group - 2) * self.tiles, self.tiles),
                    (start + self.tiles, self.tail + (group - 2) * self.rest, self.rest),
                )
            else:
                spans = ((start, self.corner + group - 4, 1),)
            self.spans.append([span for span in spans if span[2]])

    def blocks(self, group):
        out = []
        place = 0
        for _, row, count in self.spans[group]:
            pitch = self.side_rows if group < 2 else count
            out.append((row, place, count, pitch))
            place += 3 * pitch
        for passed in CARRIED.get(group, ()):
            out.append((self.corner + passed - 4, place, 1, 1))
            place += 3
        return out

    def weight_row(self, group):
        _, place, _, pitch = self.blocks(group)[-1]
        return place + 3 * pitch

    def message_rows(self, group):
        return -(-(self.weight_row(group) + self.weight_rows) // SUB) * SUB

    def lanes(self, groups, index):
        at = iota((1, LANES), 1) + index * LANES
        mine = at < 0
        for group in groups:
            for _, row, count in self.spans[group]:
                mine = mine | ((at >= row) & (at < row + count))
        return mine


def iota(shape, axis):
    return lax.broadcasted_iota(jnp.int32, shape, axis)


def arranged(points_ref, plan):
    links = points_ref.shape[1]
    width = plan.width
    raw = points_ref[...].astype(jnp.float32)
    raw = jnp.concatenate([raw, jnp.full((1, width - links), -1.0, jnp.float32)], axis=1)
    raw = jnp.broadcast_to(raw, (SUB, width))
    lane = iota((SUB, width), 1)
    row = jnp.full((SUB, width), -1.0, jnp.float32)
    for spans in plan.spans:
        for source, target, count in spans:
            turned = pltpu.roll(raw, (target - source) % width, 1)
            row = jnp.where((lane >= target) & (lane < target + count), turned, row)
    return row[0:1]


def as_column(row, rows):
    width = row.shape[1]
    shape = (rows, width)
    return jnp.sum(jnp.where(iota(shape, 0) == iota(shape, 1), row, 0.0), axis=1, keepdims=True)


def as_row(column, width):
    shape = (column.shape[0], width)
    return jnp.sum(jnp.where(iota(shape, 0) == iota(shape, 1), column[:, :1], 0.0), axis=0, keepdims=True)


def point_rows(stack, first):
    elements = stack.shape[0]
    square = (LANES, LANES)
    spread = (iota(square, 1) // SUB + first == iota(square, 0)).astype(jnp.float32)
    wide = jnp.dot(stack, spread, precision=lax.Precision.HIGHEST, preferred_element_type=jnp.float32)
    mine = iota(wide.shape, 1) % SUB == iota(wide.shape, 0) % SUB
    return jnp.sum(jnp.where(mine, wide, 0.0).reshape(elements // SUB, SUB, LANES), axis=1)


def both_halves(mass):
    return mass + pltpu.roll(mass, LANES // 2, 1)


def split_lanes(mass):
    upper = mass.astype(jnp.bfloat16).astype(jnp.float32)
    return jnp.where(iota(mass.shape, 1) < LANES // 2, mass, mass - upper)


def derive(values, axis, scale, sign=1.0):
    table, _ = gll_tables()
    out = [None] * NODES
    for other in range(4):
        spot = (lambda i: 4 * other + i) if axis == 1 else (lambda i: 4 * i + other)
        x0, x1, x2, x3 = (values[spot(i)] for i in range(4))
        diff_a = x0 - x3
        diff_b = x1 - x2
        even = (x0 + x3) - (x1 + x2)
        for i in (0, 1):
            factor = sign * scale[other] * scale[i]
            p = even * np.float32(factor * 0.5 * (table[i, 0] + table[i, 3]))
            q = diff_a * np.float32(factor * 0.5 * (table[i, 0] - table[i, 3])) + diff_b * np.float32(
                factor * 0.5 * (table[i, 1] - table[i, 2])
            )
            out[spot(i)] = q + p
            out[spot(3 - i)] = q - p
    return out


def tendency_kernel(plan, *refs):
    prog, metric, cor, points, send, recv = refs[:6]
    fields, weighted, numbers, pts_v, recv_v = refs[6:11]
    messages = refs[11:15]
    met_v, cor_v, send_v, tile, mask, total, coefs, sems, chunk_sems = refs[15:]
    elements = fields.shape[1]
    groups = elements // SUB
    chunks = 4
    cuts = chunk_sems.shape[0]
    per = elements // cuts
    smalls = [
        pltpu.make_async_copy(source, target, sems.at[i])
        for i, (source, target) in enumerate(((points, pts_v), (send, send_v), (metric, met_v), (cor, cor_v)))
    ]
    for copy in smalls:
        copy.start()
    larges = [
        pltpu.make_async_copy(
            prog.at[:, pl.ds(i * per, per)], fields.at[:, pl.ds(i * per, per)], chunk_sems.at[i]
        )
        for i in range(cuts)
    ]
    for copy in larges:
        copy.start()
    later = pltpu.make_async_copy(recv, recv_v, sems.at[4])
    later.start()
    for copy in smalls:
        copy.wait()
    rows = plan.rows
    wanted = as_column(arranged(send_v, plan), rows)
    _, scale = gll_tables()
    a, b, e, g = (met_v[i] for i in range(4))
    node = iota(a.shape, 0)
    row_edge = (node // 4 == 0) | (node // 4 == 3)
    col_edge = (node % 4 == 0) | (node % 4 == 3)
    quad = jnp.where(row_edge, np.float32(scale[0]), np.float32(scale[1])) * jnp.where(
        col_edge, np.float32(scale[0]), np.float32(scale[1])
    )
    inv = 1.0 / (a * g - b * e)
    mass = quad * inv
    share = mass * np.float32(1.0 / STEP_SIZE)
    upper = share.astype(jnp.bfloat16).astype(jnp.float32)
    stack = (a * inv, b * inv, e * inv, g * inv, mass * cor_v[...], upper, share - upper, pts_v[...].astype(jnp.float32))
    stack = jnp.transpose(jnp.concatenate(stack, axis=0))
    numbers[...] = point_rows(stack, 7 * NODES)
    step = groups // chunks
    square = (LANES, LANES)
    kind = iota(square, 0) // NODES
    half = (iota(square, 1) >= LANES // 2).astype(jnp.int32)
    lift = [(kind == i).astype(jnp.bfloat16) for i in range(5)]
    fine = jnp.concatenate(lift + [jnp.zeros(square, jnp.bfloat16)], axis=1)
    lift = jnp.concatenate([jnp.concatenate(lift + [(kind == 5 + half).astype(jnp.bfloat16)], axis=1), fine], axis=0)
    coarse = stack.astype(jnp.bfloat16).astype(jnp.float32)
    slot = iota((SUB, LANES), 1) % NODES

    def lifted(i):
        for group in range(i * step, (i + 1) * step):
            here = slice(group * SUB, (group + 1) * SUB)
            picked = jnp.concatenate(
                [
                    jnp.concatenate([jnp.where(slot == k, part[here], 0.0) for k in range(NODES)], axis=0)
                    for part in (coarse, stack - coarse)
                ],
                axis=1,
            ).astype(jnp.bfloat16)
            there = slice(group * LANES, (group + 1) * LANES)
            wide = jnp.dot(picked, lift, preferred_element_type=jnp.float32)
            for which in range(5):
                coefs[which, there, :] = wide[:, which * LANES : (which + 1) * LANES]
            weighted[there, MASS:] = wide[:, 5 * LANES :].astype(jnp.bfloat16)

    lifted(0)
    for group in range(groups):
        mask[:, group * LANES : (group + 1) * LANES] = (
            jnp.broadcast_to(wanted, (rows, LANES)) == numbers[group : group + 1, :]
        ).astype(jnp.bfloat16)

    def body(group):
        ca, cb, ce, cg, cf = (
            [coefs[i, (group * NODES + k) * SUB : (group * NODES + k + 1) * SUB, :] for k in range(NODES)]
            for i in range(5)
        )
        u, v, h = ([tile[group, f, k * SUB : (k + 1) * SUB, :] for k in range(NODES)] for f in range(3))
        span = range(NODES)
        energy = [u[k] * u[k] + v[k] * v[k] + h[k] for k in span]
        along = derive(energy, 1, scale, -0.5)
        across = derive(energy, 0, scale, -0.5)
        grad_one = [ca[k] * along[k] + ce[k] * across[k] for k in span]
        grad_two = [cb[k] * along[k] + cg[k] * across[k] for k in span]
        turn_two = derive([ca[k] * v[k] - cb[k] * u[k] for k in span], 1, scale)
        turn_one = derive([cg[k] * u[k] - ce[k] * v[k] for k in span], 0, scale)
        eta = [turn_two[k] - turn_one[k] + cf[k] for k in span]
        flow_one = derive([h[k] * (ca[k] * u[k] + cb[k] * v[k]) for k in span], 1, scale, -0.5)
        flow_two = derive([h[k] * (ce[k] * u[k] + cg[k] * v[k]) for k in span], 0, scale, -0.5)
        parts = (
            [eta[k] * v[k] + grad_one[k] for k in span],
            [grad_two[k] - eta[k] * u[k] for k in span],
            [flow_one[k] + flow_two[k] for k in span],
        )
        there = slice(group * LANES, (group + 1) * LANES)
        for f, part in enumerate(parts):
            weighted[there, f * LANES : (f + 1) * LANES] = jnp.concatenate(part, axis=0).astype(jnp.bfloat16)

    turn = (
        iota(square, 1) == iota(square, 0) % SUB * NODES + iota(square, 0) // SUB
    ).astype(jnp.bfloat16)

    def reorder(i):
        for group in range(i * step, (i + 1) * step):
            here = slice(group * SUB, (group + 1) * SUB)
            for f in range(3):
                tile[group, f] = jnp.dot(
                    turn if f < 2 else 2.0 * turn, fields[f, here].reshape(SUB * NODES, LANES), preferred_element_type=jnp.float32
                )

    def gather(i):
        span = slice(i * step * LANES, (i + 1) * step * LANES)
        part = jnp.dot(mask[:, span], weighted[span, :], preferred_element_type=jnp.float32)
        return part if i == 0 else total[...] + part

    for copy in larges:
        copy.wait()
    reorder(0)
    for i in range(chunks):
        for group in range(i * step, (i + 1) * step):
            body(group)
        if i:
            total[...] = gather(i - 1)
        if i + 1 < chunks:
            reorder(i + 1)
            lifted(i + 1)
    later.wait()
    sums = gather(chunks - 1)
    masses = as_row(both_halves(sums[:, MASS:]), plan.width)
    for group, ref in enumerate(messages):
        ref[ref.shape[0] - SUB :, :] = jnp.zeros((SUB, LANES), jnp.float32)
        for row, place, count, pitch in plan.blocks(group):
            span = pitch if pitch > count else count
            for f in range(3):
                ref[place + f * pitch : place + f * pitch + span, :] = sums[
                    row : row + span, f * LANES : (f + 1) * LANES
                ]
        for index in range(plan.weight_rows):
            mine = plan.lanes((group, *CARRIED.get(group, ())), index)
            at = plan.weight_row(group) + index
            ref[at : at + 1, :] = jnp.where(mine, masses[:, index * LANES : (index + 1) * LANES], 0.0)


def point_columns(points, group):
    return jnp.concatenate(
        [
            jnp.broadcast_to(points[:, e : e + 1], (NODES, LANES))
            for e in range(group * SUB, (group + 1) * SUB)
        ],
        axis=0,
    )


def local_sums(points, numbers, weighted, own):
    groups = weighted.shape[0] // LANES
    tall = SUB * NODES
    for i in range(own.shape[0] // tall):
        column = point_columns(points, i)
        same = jnp.concatenate(
            [(column == numbers[j : j + 1, :]).astype(jnp.bfloat16) for j in range(groups)], axis=1
        )
        own[i * tall : (i + 1) * tall, :] = jnp.dot(same, weighted[...], preferred_element_type=jnp.float32)


def local_kernel(plan, weighted, numbers, points, recv, own, table):
    landing = arranged(recv, plan)
    values = points[...].astype(jnp.float32)
    tall = SUB * NODES
    for group in range(numbers.shape[0]):
        column = point_columns(values, group)
        for i in range(0, plan.width, LANES):
            table[group * tall : (group + 1) * tall, i : i + LANES] = (
                column == landing[:, i : i + LANES]
            ).astype(jnp.bfloat16)
    local_sums(values, numbers, weighted, own)


def relay_kernel(plan, left, right, up, down):
    start = plan.weight_row(0)
    for i, ref in enumerate((up, down)):
        place = plan.blocks(0)[-2 + i][1]
        ref[0:3, :] = left[place : place + 3, :]
        ref[3:6, :] = right[place : place + 3, :]
        for index in range(plan.weight_rows):
            at = slice(start + index, start + index + 1)
            ref[6 + index : 7 + index, :] = jnp.where(
                plan.lanes(PASSED[i][:1], index), left[at, :], 0.0
            ) + jnp.where(plan.lanes(PASSED[i][1:], index), right[at, :], 0.0)


def finish_kernel(plan, fields, own, table, *refs):
    messages = refs[:4]
    relays = refs[4:6]
    out, held, landed, sems = refs[6:]
    width = plan.width
    landed[plan.tail :, :] = jnp.zeros((width - plan.tail, landed.shape[1]), jnp.float32)
    weights = []
    for index in range(plan.weight_rows):
        parts = [ref[6 + index : 7 + index, :] for ref in relays]
        for group, ref in enumerate(messages):
            at = plan.weight_row(group) + index
            row = ref[at : at + 1, :]
            parts.append(jnp.where(plan.lanes((group,), index), row, 0.0) if group < 2 else row)
        weights.append(sum(parts[1:], parts[0]))
    masses = as_column(jnp.concatenate(weights, axis=1), width)
    for group, ref in enumerate(messages):
        for row, place, count, pitch in plan.blocks(group)[: len(plan.spans[group])]:
            span = pitch if pitch > count else count
            for f in range(3):
                landed[row : row + span, f * LANES : (f + 1) * LANES] = ref[
                    place + f * pitch : place + f * pitch + span, :
                ]
    for passed, ref in zip(PASSED, relays):
        for i, group in enumerate(passed):
            row = plan.corner + group - 4
            for f in range(3):
                landed[row : row + 1, f * LANES : (f + 1) * LANES] = ref[3 * i + f : 3 * i + f + 1, :]
    landed[:, MASS:] = split_lanes(jnp.broadcast_to(masses, (width, LANES)))
    arrived = landed[...].astype(jnp.bfloat16)
    elements = fields.shape[1]
    cuts = (0, elements // 4 * 3, elements)
    copies = []
    for i in range(len(cuts) - 1):
        first, per = cuts[i], cuts[i + 1] - cuts[i]
        rows = slice(first * NODES, (first + per) * NODES)
        here = slice(first, first + per)
        total = own[rows, :] + jnp.dot(table[rows, :], arrived, preferred_element_type=jnp.float32)
        factor = 1.0 / both_halves(total[:, MASS:])
        for f in range(3):
            moved = (total[:, f * LANES : (f + 1) * LANES] * factor).reshape(per, NODES, LANES)
            held[f, here] = (fields[f, here].astype(jnp.float32) + moved).astype(jnp.bfloat16)
        copy = pltpu.make_async_copy(
            held.at[:, pl.ds(first, per)], out.at[:, pl.ds(first, per)], sems.at[i]
        )
        copy.start()
        copies.append(copy)
    for copy in copies:
        copy.wait()


def in_hbm(value):
    return pltpu.with_memory_space_constraint(value, pltpu.HBM)


def call(kernel, outs, ins, args, scratch=(), limit=8 * MIB, flops=0):
    return pl.pallas_call(
        kernel,
        out_shape=[jax.ShapeDtypeStruct(shape, dtype) for shape, dtype, _ in outs],
        out_specs=[pl.BlockSpec(memory_space=space) for _, _, space in outs],
        in_specs=[pl.BlockSpec(memory_space=space) for space in ins],
        scratch_shapes=list(scratch),
        compiler_params=pltpu.CompilerParams(vmem_limit_bytes=limit),
        cost_estimate=pl.CostEstimate(flops=flops, bytes_accessed=0, transcendentals=0) if flops else None,
    )(*args)


def local(prognostic, metric, coriolis, node_point, send_point, recv_point):
    elements = prognostic.shape[1]
    levels = prognostic.shape[3]
    links = send_point.shape[0]
    plan = Plan(elements, links, 4 * lax.axis_size("sub"))
    rows = elements * NODES
    vm, hbm = pltpu.VMEM, pltpu.HBM
    f32, bf16 = jnp.float32, jnp.bfloat16
    send = send_point.reshape(1, links)
    recv = recv_point.reshape(1, links)
    metric = jnp.transpose(metric, (0, 2, 1))
    coriolis = jnp.transpose(coriolis)
    points = jnp.transpose(node_point)
    wide = 4 * levels
    sent = call(
        lambda *refs: tendency_kernel(plan, *refs),
        (
            (prognostic.shape, bf16, vm),
            ((rows, wide), bf16, vm),
            ((elements // SUB, LANES), f32, vm),
            (points.shape, jnp.int32, vm),
            (recv.shape, jnp.int32, vm),
        )
        + tuple(((plan.message_rows(group), LANES), f32, vm) for group in range(4)),
        (hbm,) * 6,
        tuple(in_hbm(x) for x in (prognostic, metric, coriolis, points, send, recv)),
        (
            vm(metric.shape, f32),
            vm(coriolis.shape, f32),
            vm(send.shape, jnp.int32),
            vm((elements // SUB, 3, SUB * NODES, levels), f32),
            vm((plan.rows, rows), bf16),
            vm((plan.rows, wide), f32),
            vm((5, rows, LANES), f32),
            pltpu.SemaphoreType.DMA((5,)),
            pltpu.SemaphoreType.DMA((1,)),
        ),
    )
    fields, weighted, numbers, points, recv = sent[:5]
    landed = []
    for group in range(4):
        landed.append(shift(sent[5 + group], plan.offsets[group]))
    own, table = call(
        lambda *refs: local_kernel(plan, *refs),
        (((rows, wide), f32, vm), ((rows, plan.width), bf16, vm)),
        (vm,) * 4,
        (weighted, numbers, points, recv),
    )
    relays = call(
        lambda *refs: relay_kernel(plan, *refs), (((SUB, LANES), f32, vm),) * 2, (vm, vm), (landed[0], landed[1])
    )
    passed = []
    for i, offset in enumerate((plan.lap, -plan.lap)):
        passed.append(shift(relays[i], offset))
    (advanced,) = call(
        lambda *refs: finish_kernel(plan, *refs),
        ((prognostic.shape, bf16, hbm),),
        (vm,) * 9,
        (fields, own, table, *landed, *passed),
        (
            vm(prognostic.shape, bf16),
            vm((plan.width, wide), f32),
            pltpu.SemaphoreType.DMA((2,)),
        ),
    )
    return advanced


def solution(mesh):
    placed = (
        P(None, AXES, None, None),
        P(None, AXES, None),
        P(AXES, None),
        P(AXES, None),
        P(AXES),
        P(AXES),
    )
    return jax.shard_map(
        local,
        mesh=mesh,
        in_specs=placed,
        out_specs=P(None, AXES, None, None),
        check_vma=False,
    )
```
